1024 devices in a mesh: own: 16 (over y, x_hi), rep: 64 (over x_lo, z, core).
Axes of the slice: x: 4 (x_hi: 2, x_lo: 2; x = x_hi * 2 + x_lo), y: 8, z: 16, core: 2. Of those that a mesh axis runs over, the one named last changes fastest.
Arguments:
- tokens: bfloat16 [131072, 2048], P(('own', 'rep')), may hold values from -6 to 6
- cotangent: bfloat16 [131072, 2048], P(('own', 'rep')), may hold values from -3 to 3
- route: int32 [131072, 1], P(('own', 'rep')), may hold values from 0 to 63; in each aligned block of 128 rows (0 to 127, 128 to 255, ...) at most 3 rows name the same one
- host: int32 [64], replicated, may hold values from 0 to 63, each once
- w_gate: bfloat16 [64, 2048, 256], P('rep', 'own'), may hold values from -0.125 to 0.125
- w_up: bfloat16 [64, 2048, 256], P('rep', 'own'), may hold values from -0.125 to 0.125
- w_down_t: bfloat16 [64, 2048, 256], P('rep', 'own'), may hold values from -0.375 to 0.375
Outputs:
- x_grad: bfloat16 [131072, 2048], P(('own', 'rep'))
- grad_gate: float32 [64, 2048, 256], P('rep', 'own')
- grad_up: float32 [64, 2048, 256], P('rep', 'own')
- grad_down_t: float32 [64, 2048, 256], P('rep', 'own')
The draws below stay inside these ranges and needn't reach their ends.
Inputs may be any that keep to these rules, and one draw needn't show every extreme that they name: `route`: among the 128 tokens of one device no hot expert is named more than 3 times, and in every draw some expert is named exactly 3 times on some device. `host`: each replica group serves exactly one hot expert.
All inputs are finite; a program needn't handle non-finite values.
Results may differ from the reference program's by a relative error of at most 0.017.
Values may be sent and summed in bfloat16 or wider, within the bound.
A program may use at most 32 MiB of HBM per device.

```python
import math
import jax
import jax.numpy as jnp
import numpy as np
from jax import lax

D = 2048
HW = 256
TOK_DEV = 128
HOT = 64
CAP = 3
TOKENS = 131072
N_OWN = 16
N_REP = 64


def shard_levels(rng, dims, shards, smallest, high):
    def one(dim, shards_of):
        draws = jax.random.uniform(jax.random.fold_in(jax.random.fold_in(rng, 6), dim), (shards_of,), jnp.float32, smallest / len(shards), high / len(shards))
        return jnp.repeat(jnp.exp(draws), dims[dim] // shards_of).reshape((-1,) + (1,) * (len(dims) - dim - 1))

    factor_of = one(*shards[0])
    for cut in shards[1:]:
        factor_of = factor_of * one(*cut)
    return factor_of


def assign_block(rng, own, number, rows, number_of, top, reach, skew):
    ranking = jax.random.permutation(rng, number_of)
    crowded, usual = load_shares(number_of, rows * top, reach, skew, True), load_shares(number_of, rows * top, reach, skew, False)
    places = jnp.arange(number_of)

    def named(sizes, offset_by):
        used = int((sizes > 0).sum())
        fixed = max(1, used // 4)
        passed = fixed + (places - fixed + offset_by * (used - fixed)) % max(1, number_of - fixed)
        return jnp.zeros((number_of,), jnp.int32).at[ranking[jnp.where(places < fixed, places, passed)]].set(jnp.asarray(sizes, jnp.int32))

    sizes = jnp.where(number % 4 == 0, named(crowded, number // 4), named(usual, number - number // 4 - 1))
    mixed = jax.random.permutation(jax.random.fold_in(own, 3), number_of)
    donor, receiver = mixed[0:number_of // 2 * 2:2], mixed[1:number_of // 2 * 2:2]
    margin = jnp.minimum(sizes[donor] - 1, reach - sizes[receiver]) // 2
    margin = jnp.where((donor == ranking[0]) | (receiver == ranking[0]) | (sizes[receiver] == 0), 0, jnp.maximum(margin, 0))
    passed = jax.random.randint(jax.random.fold_in(own, 4), (number_of // 2,), 0, 1 << 20) % (margin + 1)
    sizes = sizes.at[donor].add(-passed).at[receiver].add(passed)
    items = jnp.searchsorted(jnp.cumsum(sizes), jnp.arange(rows * top), side="right").astype(jnp.int32)
    grid = items.reshape(top, rows).T
    grid = grid[jax.random.permutation(jax.random.fold_in(own, 1), rows)]
    offset_by = jax.random.randint(jax.random.fold_in(own, 2), (rows, 1), 0, top)
    return jnp.take_along_axis(grid, (jnp.arange(top)[None, :] + offset_by) % top, axis=1)


def load_shares(count, total, limit, lean, full):
    portions = [(1 << 20) // math.isqrt(grade ** lean) + 1 for grade in range(1, count + 1)]
    largest = limit if full else min(limit, max(-(-total // count), total * portions[0] // sum(portions)))
    least = 1 if total - largest >= count - 1 else 0
    given, spare = [largest] + [least] * (count - 1), total - largest - least * (count - 1)
    while spare > 0:
        free = [i for i in range(1, count) if given[i] < largest] or [i for i in range(1, count) if given[i] < limit]
        pool, remaining = sum([portions[i] for i in free]), spare
        for i in free:
            addition = min(limit - given[i], max(1, remaining * portions[i] // pool), spare)
            given[i] = given[i] + addition
            spare = spare - addition
    return np.array(given)


def scatter_about(rng, extent, spread, most, pieces=(), kind=jnp.bfloat16):
    drawn = jax.random.normal(rng, extent, jnp.float32) * spread
    if len(pieces) > 0:
        drawn = shard_levels(rng, extent, pieces, -0.22, 0.18) * drawn
    return jnp.clip(drawn, min=-most, max=most).astype(kind)


def setup_inputs(seed: int = 0) -> dict:
    key_of = jax.random.split(jax.random.key(seed), 8)
    tokens = scatter_about(key_of[0], (TOKENS, D), 1.0, 6.0, ((0, 1024),))
    cotangent = scatter_about(key_of[1], (TOKENS, D), 0.5, 3.0, ((0, 1024),))
    route_keys = jax.random.split(jax.random.fold_in(key_of[2], 1), TOKENS // TOK_DEV)
    route_turns = jax.random.permutation(jax.random.fold_in(key_of[2], 3), TOKENS // TOK_DEV)
    route = jax.vmap(lambda own, number: assign_block(jax.random.fold_in(key_of[2], 2), own, number, TOK_DEV, HOT, 1, CAP, 2))(route_keys, route_turns).reshape((TOKENS, 1))
    host = jax.random.permutation(key_of[3], HOT).astype(jnp.int32)
    w_gate = scatter_about(key_of[4], (HOT, D, HW), D ** -0.5, 0.125, ((0, 64), (1, 16)))
    w_up = scatter_about(key_of[5], (HOT, D, HW), D ** -0.5, 0.125, ((0, 64), (1, 16)))
    w_down_t = scatter_about(key_of[6], (HOT, D, HW), HW ** -0.5, 0.375, ((0, 64), (1, 16)))
    return {"tokens": tokens, "cotangent": cotangent, "route": route, "host": host, "w_gate": w_gate, "w_up": w_up, "w_down_t": w_down_t}


def reference(tokens, cotangent, route, host, w_gate, w_up, w_down_t):
    target = host[route[:, 0]].reshape(N_OWN, N_REP, TOK_DEV)
    labels = jnp.arange(HOT, dtype=jnp.int32)
    marked = (target[..., None] == labels).astype(jnp.int32)
    arrival = (jnp.sum(jnp.cumsum(marked, axis=2) * marked, axis=3) - 1).astype(jnp.int32)
    x_all = tokens.reshape(N_OWN, N_REP, TOK_DEV, D)
    dy_all = cotangent.reshape(N_OWN, N_REP, TOK_DEV, D)
    source = jnp.broadcast_to(jnp.arange(N_REP, dtype=jnp.int32)[:, None], (N_REP, TOK_DEV))
    gate_f = w_gate.astype(jnp.float32)
    up_f = w_up.astype(jnp.float32)
    down_f = w_down_t.astype(jnp.float32)

    def per_row(totals, item):
        x_row, dy_row, target_row, arrival_row = item
        empty = jnp.zeros((HOT, N_REP, CAP, D), jnp.bfloat16)
        slot_x = empty.at[target_row, source, arrival_row].set(x_row).reshape(HOT, N_REP * CAP, D).astype(jnp.float32)
        slot_dy = empty.at[target_row, source, arrival_row].set(dy_row).reshape(HOT, N_REP * CAP, D).astype(jnp.float32)
        gate_act = jnp.einsum("esd,edh->esh", slot_x, gate_f)
        up_act = jnp.einsum("esd,edh->esh", slot_x, up_f)
        back_grad = jnp.einsum("esd,edh->esh", slot_dy, down_f)
        sigmoid_g = jax.nn.sigmoid(gate_act)
        silu_gate = gate_act * sigmoid_g
        hidden = (silu_gate * up_act).astype(jnp.bfloat16).astype(jnp.float32)
        grad_gate_h = (back_grad * up_act * sigmoid_g * (1.0 + gate_act * (1.0 - sigmoid_g))).astype(jnp.bfloat16).astype(jnp.float32)
        grad_up_h = (back_grad * silu_gate).astype(jnp.bfloat16).astype(jnp.float32)
        slot_grad = jnp.einsum("esh,edh->esd", grad_gate_h, gate_f) + jnp.einsum("esh,edh->esd", grad_up_h, up_f)
        slot_grad = slot_grad.astype(jnp.bfloat16).reshape(HOT, N_REP, CAP, D)
        x_back = slot_grad[target_row, source, arrival_row]
        partial_terms = jnp.stack([
            jnp.einsum("esd,esh->edh", slot_x, grad_gate_h),
            jnp.einsum("esd,esh->edh", slot_x, grad_up_h),
            jnp.einsum("esd,esh->edh", slot_dy, hidden)]).astype(jnp.bfloat16)
        partial_terms = lax.optimization_barrier(partial_terms)
        return totals + partial_terms.astype(jnp.float32), x_back

    start = jnp.zeros((3, HOT, D, HW), jnp.float32)
    totals, x_back = lax.scan(per_row, start, (x_all, dy_all, target, arrival))
    return x_back.reshape(TOKENS, D), totals[0], totals[1], totals[2]
```

```python
import functools

import jax
import jax.numpy as jnp
from jax import lax
from jax.experimental import pallas as pl
from jax.experimental.pallas import tpu as pltpu
from jax.sharding import PartitionSpec as P

MESH = pl.DeviceIdType.MESH
CAP = 3
CORES = 2
X_LO = 2
X_HI = 2


def nn(left, right):
    return lax.dot_general(
        left, right, (((1,), (0,)), ((), ())), preferred_element_type=jnp.float32
    )


def nt(left, right):
    return lax.dot_general(
        left, right, (((1,), (1,)), ((), ())), preferred_element_type=jnp.float32
    )


def tn(left, right):
    return lax.dot_general(
        left, right, (((0,), (0,)), ((), ())), preferred_element_type=jnp.float32
    )


def kernel(
    n_own,
    n_rep,
    src_ref,
    pos_ref,
    tok_ref,
    cot_ref,
    wg_ref,
    wu_ref,
    wd_ref,
    xg_ref,
    gg_ref,
    gu_ref,
    gd_ref,
    send,
    recv,
    weights,
    wide,
    xs,
    dys,
    grads_h,
    hidden_s,
    back,
    returned,
    stage,
    chain,
    cross,
    crossed,
    local_sem,
    a2a_send,
    a2a_recv,
    ret_send,
    ret_recv,
    agx_send,
    agx_recv,
    ag_send,
    ag_recv,
    rs_send,
    rs_recv,
    rsx_send,
    rsx_recv,
):
    n_y = n_own // X_HI
    n_z = n_rep // (X_LO * CORES)
    half = n_y // 2
    rows = n_rep * CAP
    me_o = lax.axis_index("own")
    me_r = lax.axis_index("rep")
    y = me_o // X_HI
    xh = lax.rem(me_o, X_HI)
    xl = me_r // (n_z * CORES)
    z = lax.rem(me_r // CORES, n_z)
    core = lax.rem(me_r, CORES)

    def own_at(dy, h):
        return lax.rem(y + dy + n_y, n_y) * X_HI + h

    right = (own_at(1, xh), me_r)
    left = (own_at(-1, xh), me_r)
    partner = (y * X_HI + (1 - xh), me_r)
    towards = (right, left)

    def rep_at(dz, dxl, dc):
        return (
            lax.rem(xl + dxl, X_LO) * (n_z * CORES)
            + lax.rem(z + dz + n_z, n_z) * CORES
            + lax.rem(core + dc, CORES)
        )

    def each_peer(body):
        def far(k, carry):
            distance = n_z // 2 - (k + 1) // 2
            dz = jnp.where(lax.rem(k, 2) == 0, -distance, distance)
            for dxl in range(X_LO):
                for dc in range(CORES):
                    body(rep_at(dz, dxl, dc))
            return carry

        lax.fori_loop(0, n_z - 1, far, 0)
        for dxl in range(X_LO):
            for dc in range(CORES):
                if dxl or dc:
                    body(rep_at(0, dxl, dc))

    for k, w_ref in enumerate((wg_ref, wu_ref, wd_ref)):
        pltpu.make_async_copy(w_ref.at[0], weights.at[me_o, k], local_sem.at[k]).start()

    barrier = pltpu.get_barrier_semaphore()
    for dev in (right, left, partner):
        pl.semaphore_signal(barrier, inc=1, device_id=dev, device_id_type=MESH)
    each_peer(
        lambda r: pl.semaphore_signal(
            barrier, inc=1, device_id=(me_o, r), device_id_type=MESH
        )
    )

    def fill(s, carry):
        for c in range(CAP):
            row = src_ref[s * CAP + c]
            send[s * 2 * CAP + c] = tok_ref[row]
            send[s * 2 * CAP + CAP + c] = cot_ref[row]
        return carry

    lax.fori_loop(0, n_rep, fill, 0)
    for k, w_ref in enumerate((wg_ref, wu_ref, wd_ref)):
        pltpu.make_async_copy(w_ref.at[0], weights.at[me_o, k], local_sem.at[k]).wait()
    pl.semaphore_wait(barrier, n_rep - 1 + 3)

    def weight_copy(block, dev, s_sem, r_sem):
        return pltpu.make_async_remote_copy(
            src_ref=weights.at[block],
            dst_ref=weights.at[block],
            send_sem=s_sem,
            recv_sem=r_sem,
            device_id=dev,
            device_id_type=MESH,
        )

    partner_copy = weight_copy(me_o, partner, agx_send, agx_recv)
    partner_copy.start()

    def ring_copy(way, s, other):
        h = (1 - xh) if other else xh
        block = own_at(-s if way == 0 else s, h)
        return weight_copy(
            block,
            towards[way],
            ag_send.at[way, s, int(other)],
            ag_recv.at[way, s, int(other)],
        )

    def ring_hops(s):
        if s < half - 1:
            return [(way, s, other) for other in (False, True) for way in (0, 1)]
        return [(0, s, False), (1, s, True)]

    for way in (0, 1):
        if (way, 0, False) in ring_hops(0):
            ring_copy(way, 0, False).start()

    def token_copy(r):
        return pltpu.make_async_remote_copy(
            src_ref=send.at[pl.ds(r * 2 * CAP, 2 * CAP)],
            dst_ref=recv.at[pl.ds(me_r * 2 * CAP, 2 * CAP)],
            send_sem=a2a_send,
            recv_sem=a2a_recv,
            device_id=(me_o, r),
            device_id_type=MESH,
        )

    each_peer(lambda r: token_copy(r).start())
    self_copy = pltpu.make_async_copy(
        send.at[pl.ds(me_r * 2 * CAP, 2 * CAP)],
        recv.at[pl.ds(me_r * 2 * CAP, 2 * CAP)],
        local_sem.at[0],
    )
    self_copy.start()

    partner_copy.wait()
    for way in (0, 1):
        if (way, 0, True) in ring_hops(0):
            ring_copy(way, 0, True).start()
    for s in range(half):
        for way, s_, other in ring_hops(s):
            ring_copy(way, s, other).wait_recv()
            if s + 1 < half and (way, s + 1, other) in ring_hops(s + 1):
                ring_copy(way, s + 1, other).start()

    self_copy.wait()

    def whole(buffer, sem, per_peer):
        view = buffer.at[pl.ds(0, (n_rep - 1) * per_peer)]
        return pltpu.make_async_copy(view, view, sem)

    whole(recv, a2a_recv, 2 * CAP).wait()

    def widen(r, carry):
        block = recv[pl.ds(r * 2 * CAP, 2 * CAP)].astype(jnp.float32)
        at = r * CAP * n_own
        for c in range(CAP):
            wide[0, pl.ds(at + c * n_own, n_own), :] = block[c]
            wide[1, pl.ds(at + c * n_own, n_own), :] = block[CAP + c]
        return carry

    lax.fori_loop(0, n_rep, widen, 0)

    gate = jnp.zeros((rows, wg_ref.shape[2]), jnp.float32)
    up = jnp.zeros_like(gate)
    grad_back = jnp.zeros_like(gate)
    for p in range(n_y):
        pair = [
            jnp.concatenate(
                [
                    wide[i, pl.ds(X_HI * p + h, rows, stride=n_own), :].astype(jnp.bfloat16)
                    for h in range(X_HI)
                ],
                axis=1,
            )
            for i in range(2)
        ]
        xs[p] = pair[0]
        dys[p] = pair[1]
        w_of = [
            jnp.concatenate([weights[X_HI * p + h, k] for h in range(X_HI)], axis=0)
            for k in range(3)
        ]
        gate += nn(pair[0], w_of[0])
        up += nn(pair[0], w_of[1])
        grad_back += nn(pair[1], w_of[2])

    sg = jax.nn.sigmoid(gate)
    silu = gate * sg
    hidden_s[...] = (silu * up).astype(jnp.bfloat16)
    hw = gate.shape[1]
    grads_h[:, :hw] = (grad_back * up * sg * (1.0 + gate * (1.0 - sg))).astype(jnp.bfloat16)
    grads_h[:, hw:] = (grad_back * silu).astype(jnp.bfloat16)

    for p in range(n_y):
        for h in range(X_HI):
            j = X_HI * p + h
            part = nt(grads_h[:, :hw], weights[j, 0]) + nt(grads_h[:, hw:], weights[j, 1])
            wide[0, pl.ds(j, rows, stride=n_own), :] = part

    def narrow(r, carry):
        for c in range(CAP):
            at = (r * CAP + c) * n_own
            back[r * CAP + c] = wide[0, pl.ds(at, n_own), :].astype(jnp.bfloat16)
        return carry

    lax.fori_loop(0, n_rep, narrow, 0)

    def return_copy(r):
        return pltpu.make_async_remote_copy(
            src_ref=back.at[pl.ds(r * CAP, CAP)],
            dst_ref=returned.at[pl.ds(me_r * CAP, CAP)],
            send_sem=ret_send,
            recv_sem=ret_recv,
            device_id=(me_o, r),
            device_id_type=MESH,
        )

    each_peer(lambda r: return_copy(r).start())
    back_copy = pltpu.make_async_copy(
        back.at[pl.ds(me_r * CAP, CAP)],
        returned.at[pl.ds(me_r * CAP, CAP)],
        local_sem.at[0],
    )
    back_copy.start()

    def terms(dy):
        p = lax.rem(y + dy + n_y, n_y)
        both = tn(xs[p], grads_h[...])
        down = tn(dys[p], hidden_s[...])
        size = both.shape[0] // X_HI
        out = []
        for h in range(X_HI):
            piece = slice(h * size, (h + 1) * size)
            out.append([both[piece, :hw], both[piece, hw:], down[piece]])
        return out

    def sum_copy(way, s, h):
        return pltpu.make_async_remote_copy(
            src_ref=stage.at[way, s, h],
            dst_ref=chain.at[way, s, h],
            send_sem=rs_send.at[way, s, h],
            recv_sem=rs_recv.at[way, s, h],
            device_id=towards[way],
            device_id_type=MESH,
        )

    def columns(way, s):
        return range(X_HI) if s > 0 else (way,)

    for s in range(half):
        shared = terms(half) if s == 0 else None
        for way in (0, 1):
            distance = half - s
            local = shared or terms(distance if way == 0 else -distance)
            for h in columns(way, s):
                arrived = s > 0 and h in columns(way, s - 1)
                if arrived:
                    sum_copy(way, s - 1, h).wait_recv()
                for k in range(3):
                    value = local[h][k].astype(jnp.bfloat16)
                    if arrived:
                        value = (
                            value.astype(jnp.float32)
                            + chain[way, s - 1, h, k].astype(jnp.float32)
                        ).astype(jnp.bfloat16)
                    stage[way, s, h, k] = value
                sum_copy(way, s, h).start()

    local = terms(0)
    for h in range(X_HI):
        for k in range(3):
            wide[1, pl.ds((h * 3 + k) * 2 * local[h][k].shape[0], 2 * local[h][k].shape[0]), :] = (
                jnp.concatenate([local[h][k][:, :128], local[h][k][:, 128:]], axis=0)
                .astype(jnp.bfloat16)
                .astype(jnp.float32)
            )
    size = wg_ref.shape[1]

    def summed(h, k):
        at = (h * 3 + k) * 2 * size
        low = wide[1, pl.ds(at, size), :]
        high = wide[1, pl.ds(at + size, size), :]
        total = jnp.concatenate([low, high], axis=1)
        for way in (0, 1):
            total += chain[way, half - 1, h, k].astype(jnp.float32)
        return total

    for h in range(X_HI):
        for way in (0, 1):
            if h in columns(way, half - 1):
                sum_copy(way, half - 1, h).wait_recv()

    for k in range(3):
        cross[k] = jnp.where(xh == 0, summed(1, k), summed(0, k)).astype(jnp.bfloat16)
    cross_copy = pltpu.make_async_remote_copy(
        src_ref=cross,
        dst_ref=crossed,
        send_sem=rsx_send,
        recv_sem=rsx_recv,
        device_id=partner,
        device_id_type=MESH,
    )
    cross_copy.start()

    back_copy.wait()
    whole(returned, ret_recv, CAP).wait()

    def pick(t, carry):
        xg_ref[t] = returned[pos_ref[t]]
        return carry

    lax.fori_loop(0, xg_ref.shape[0], pick, 0)

    cross_copy.wait()
    for k, out in enumerate((gg_ref, gu_ref, gd_ref)):
        out[0] = jnp.where(xh == 0, summed(0, k), summed(1, k)) + crossed[k].astype(jnp.float32)

    whole(send, a2a_send, 2 * CAP).wait()
    whole(back, ret_send, CAP).wait()
    for s in range(half):
        for way, s_, other in ring_hops(s):
            ring_copy(way, s, other).wait_send()
        for way in (0, 1):
            for h in columns(way, s):
                sum_copy(way, s, h).wait_send()


def shards(n_own, n_rep, tokens, cotangent, route, host, w_gate, w_up, w_down_t):
    tok_rows, width = tokens.shape
    hw = w_gate.shape[2]
    piece = w_gate.shape[1]
    lanes = width // n_own
    rows = n_rep * CAP
    labels = lax.broadcasted_iota(jnp.int32, (tok_rows, n_rep), 1)
    target = jnp.sum(jnp.where(route == labels, host[None, :], 0), axis=1)
    earlier = lax.broadcasted_iota(jnp.int32, (tok_rows, tok_rows), 1) < lax.broadcasted_iota(
        jnp.int32, (tok_rows, tok_rows), 0
    )
    arrival = jnp.sum(
        jnp.where((target[:, None] == target[None, :]) & earlier, 1, 0), axis=1
    )
    position = target * CAP + arrival
    slot_ids = lax.broadcasted_iota(jnp.int32, (rows, tok_rows), 0)
    token_ids = lax.broadcasted_iota(jnp.int32, (rows, tok_rows), 1)
    source = tok_rows + jnp.sum(
        jnp.where(slot_ids == position[None, :], token_ids - tok_rows, 0), axis=1
    )
    tok = jnp.pad(tokens.reshape(tok_rows, n_own, lanes), ((0, 1), (0, 0), (0, 0)))
    cot = jnp.pad(cotangent.reshape(tok_rows, n_own, lanes), ((0, 1), (0, 0), (0, 0)))

    bf16, f32 = jnp.bfloat16, jnp.float32
    half = n_own // X_HI // 2
    vmem = pl.BlockSpec(memory_space=pltpu.VMEM)
    smem = pl.BlockSpec(memory_space=pltpu.SMEM)
    dma = pltpu.SemaphoreType.DMA
    x_rows, gate, up, down = pl.pallas_call(
        functools.partial(kernel, n_own, n_rep),
        out_shape=(
            jax.ShapeDtypeStruct((tok_rows, n_own, lanes), bf16),
            jax.ShapeDtypeStruct((1, piece, hw), f32),
            jax.ShapeDtypeStruct((1, piece, hw), f32),
            jax.ShapeDtypeStruct((1, piece, hw), f32),
        ),
        in_specs=[smem, smem] + [vmem] * 5,
        out_specs=(vmem,) * 4,
        scratch_shapes=[
            pltpu.VMEM((2 * rows, n_own, lanes), bf16),
            pltpu.VMEM((2 * rows, n_own, lanes), bf16),
            pltpu.VMEM((n_own, 3, piece, hw), bf16),
            pltpu.VMEM((2, max(rows * n_own, 12 * piece), lanes), f32),
            pltpu.VMEM((n_own // X_HI, rows, X_HI * lanes), bf16),
            pltpu.VMEM((n_own // X_HI, rows, X_HI * lanes), bf16),
            pltpu.VMEM((rows, 2 * hw), bf16),
            pltpu.VMEM((rows, hw), bf16),
            pltpu.VMEM((rows, n_own, lanes), bf16),
            pltpu.VMEM((rows, n_own, lanes), bf16),
            pltpu.VMEM((2, half, X_HI, 3, piece, hw), bf16),
            pltpu.VMEM((2, half, X_HI, 3, piece, hw), bf16),
            pltpu.VMEM((3, piece, hw), bf16),
            pltpu.VMEM((3, piece, hw), bf16),
            dma((3,)),
            dma,
            dma,
            dma,
            dma,
            dma,
            dma,
            dma((2, half, 2)),
            dma((2, half, 2)),
            dma((2, half, 2)),
            dma((2, half, 2)),
            dma,
            dma,
        ],
        compiler_params=pltpu.CompilerParams(collective_id=0, has_side_effects=True),
    )(source, position, tok, cot, w_gate, w_up, w_down_t)
    return (x_rows.reshape(tok_rows, width), gate, up, down)


def solution(mesh):
    body = functools.partial(shards, mesh.shape["own"], mesh.shape["rep"])
    return jax.shard_map(
        body,
        mesh=mesh,
        in_specs=(
            P(("own", "rep"), None),
            P(("own", "rep"), None),
            P(("own", "rep"), None),
            P(),
            P("rep", "own", None),
            P("rep", "own", None),
            P("rep", "own", None),
        ),
        out_specs=(
            P(("own", "rep"), None),
            P("rep", "own", None),
            P("rep", "own", None),
            P("rep", "own", None),
        ),
        check_vma=False,
    )
```

```python
import functools

import jax
import jax.numpy as jnp
from jax import lax
from jax.experimental import pallas as pl
from jax.experimental.pallas import tpu as pltpu
from jax.sharding import PartitionSpec as P

MESH = pl.DeviceIdType.MESH
CAP = 3
CORES = 2
X_LO = 2
X_HI = 2


def nn(left, right):
    return lax.dot_general(
        left, right, (((1,), (0,)), ((), ())), preferred_element_type=jnp.float32
    )


def nt(left, right):
    return lax.dot_general(
        left, right, (((1,), (1,)), ((), ())), preferred_element_type=jnp.float32
    )


def tn(left, right):
    return lax.dot_general(
        left, right, (((0,), (0,)), ((), ())), preferred_element_type=jnp.float32
    )


def kernel(
    n_own,
    n_rep,
    src_ref,
    pos_ref,
    tok_ref,
    cot_ref,
    wg_ref,
    wu_ref,
    wd_ref,
    xg_ref,
    sums_ref,
    tok_in,
    x_of,
    dy_of,
    send,
    recv,
    weights,
    wide,
    xs,
    dys,
    grads_h,
    hidden_s,
    back,
    returned,
    stage,
    chain,
    total,
    cross,
    crossed,
    relay_rows,
    relay_back,
    local_sem,
    ready,
    relay_in,
    relay_out,
    relay_back_in,
    relay_back_out,
    a2a_send,
    a2a_recv,
    ret_send,
    ret_recv,
    agx_send,
    agx_recv,
    ag_send,
    ag_recv,
    rs_send,
    rs_recv,
    rsx_send,
    rsx_recv,
):
    n_y = n_own // X_HI
    n_z = n_rep // (X_LO * CORES)
    half = n_y // 2
    plane = X_LO * CORES
    far = n_z // 2
    quarter = n_z // 4
    group = n_rep // 2
    rows = group * CAP
    hw = wg_ref.shape[2]
    toks = tok_ref.shape[0]
    lanes = tok_ref.shape[1] // n_own
    me_o = lax.axis_index("own")
    me_r = lax.axis_index("rep")
    y = me_o // X_HI
    xh = lax.rem(me_o, X_HI)
    xl = me_r // (n_z * CORES)
    z = lax.rem(me_r // CORES, n_z)
    core = lax.rem(me_r, CORES)

    def own_at(dy, h):
        return lax.rem(y + dy + n_y, n_y) * X_HI + h

    right = (own_at(1, xh), me_r)
    left = (own_at(-1, xh), me_r)
    partner = (y * X_HI + (1 - xh), me_r)
    towards = (right, left)

    def rep_at(dz, dxl, dc):
        return (
            lax.rem(xl + dxl, X_LO) * (n_z * CORES)
            + lax.rem(z + dz + n_z, n_z) * CORES
            + lax.rem(core + dc, CORES)
        )

    def signal(sem, dev):
        pl.semaphore_signal(sem, inc=1, device_id=dev, device_id_type=MESH)

    in_plane = [(dxl, dc) for dxl in range(X_LO) for dc in range(CORES)]
    ahead = (me_o, rep_at(1, 0, 0))
    behind = (me_o, rep_at(-1, 0, 0))
    barrier = pltpu.get_barrier_semaphore()
    for dev in (right, left, partner, ahead, behind):
        signal(barrier, dev)
    for dxl, dc in in_plane[1:]:
        signal(barrier, (me_o, rep_at(0, dxl, dc)))

    loads = [
        pltpu.make_async_copy(ref, tok_in.at[i], local_sem.at[3 + i])
        for i, ref in enumerate((tok_ref, cot_ref))
    ] + [
        pltpu.make_async_copy(w_ref.at[0], weights.at[me_o, k], local_sem.at[k])
        for k, w_ref in enumerate((wg_ref, wu_ref, wd_ref))
    ]
    for copy in loads:
        copy.start()

    for i in range(2):
        loads[i].wait()
        for j in range(n_own):
            wide[i, pl.ds(j, toks, stride=n_own), :] = tok_in[
                i, :, j * lanes : (j + 1) * lanes
            ].astype(jnp.float32)

    def by_token(t, carry):
        at = pl.ds(pl.multiple_of(t * n_own, n_own), n_own)
        x_of[t] = wide[0, at, :].astype(jnp.bfloat16)
        dy_of[t] = wide[1, at, :].astype(jnp.bfloat16)
        return carry

    lax.fori_loop(0, toks, by_token, 0, unroll=4)
    for rows_of in (x_of, dy_of):
        rows_of[toks] = jnp.zeros((n_own, lanes), jnp.bfloat16)

    def fill(s, carry):
        for c in range(CAP):
            row = src_ref[s * CAP + c]
            send[s * 2 * CAP + c] = x_of[row]
            send[s * 2 * CAP + CAP + c] = dy_of[row]
        return carry

    lax.fori_loop(0, n_rep, fill, 0)
    for copy in loads[2:]:
        copy.wait()
    pl.semaphore_wait(barrier, 5 + plane - 1)

    signal(ready.at[0, 0], ahead)
    signal(ready.at[1, 0], behind)

    def weight_copy(block, dev, s_sem, r_sem):
        return pltpu.make_async_remote_copy(
            src_ref=weights.at[block],
            dst_ref=weights.at[block],
            send_sem=s_sem,
            recv_sem=r_sem,
            device_id=dev,
            device_id_type=MESH,
        )

    partner_copy = weight_copy(me_o, partner, agx_send, agx_recv)
    partner_copy.start()

    def ring_copy(way, s, other):
        h = (1 - xh) if other else xh
        block = own_at(-s if way == 0 else s, h)
        return weight_copy(
            block,
            towards[way],
            ag_send.at[way, s, int(other)],
            ag_recv.at[way, s, int(other)],
        )

    def ring_hops(s):
        if s < half - 1:
            return [(way, s, other) for other in (False, True) for way in (0, 1)]
        return [(0, s, False), (1, s, True)]

    for way in (0, 1):
        if (way, 0, False) in ring_hops(0):
            ring_copy(way, 0, False).start()

    def send_plane(dz, at, members):
        for dxl, dc in members:
            r = rep_at(dz, dxl, dc)
            place = at * plane + dxl * CORES + dc
            pltpu.make_async_remote_copy(
                src_ref=send.at[pl.ds(r * 2 * CAP, 2 * CAP)],
                dst_ref=recv.at[pl.ds(place * 2 * CAP, 2 * CAP)],
                send_sem=a2a_send,
                recv_sem=a2a_recv.at[at // far],
                device_id=(me_o, r),
                device_id_type=MESH,
            ).start()

    send_plane(0, 0, in_plane[1:])
    self_copy = pltpu.make_async_copy(
        send.at[pl.ds(me_r * 2 * CAP, 2 * CAP)],
        recv.at[pl.ds(0, 2 * CAP)],
        local_sem.at[0],
    )
    self_copy.start()

    def send_both(d, forward):
        for way, ahead_of in enumerate((ahead, behind)):
            pl.semaphore_wait(ready.at[way, d - 1], 1)
            if forward:
                signal(ready.at[way, d], ahead_of)
        send_plane(d, 2 * d, in_plane)
        send_plane(-d, 2 * d - 1, in_plane)

    def send_planes(first, last):
        def one(d, carry):
            send_both(d, True)
            return carry

        lax.fori_loop(first, min(last + 1, far - 1), one, 0)
        if last == far - 1:
            send_both(last, False)

    ways = [(0, quarter), (1, -quarter)]
    crossing = [(way, dz, dxl) for way, dz in ways for dxl in range(X_LO)]

    def via(src, dst, s_sem, r_sem, dz):
        pltpu.make_async_remote_copy(
            src_ref=src,
            dst_ref=dst,
            send_sem=s_sem,
            recv_sem=r_sem,
            device_id=(me_o, rep_at(dz, 0, 0)),
            device_id_type=MESH,
        ).start()

    send_planes(1, quarter)
    for way, dz, dxl in crossing:
        r = rep_at(far, dxl, way)
        via(
            send.at[pl.ds(r * 2 * CAP, 2 * CAP)],
            relay_rows.at[pl.ds((way * X_LO + dxl) * 2 * CAP, 2 * CAP)],
            a2a_send,
            relay_in,
            dz,
        )
    if quarter < far - 1:
        send_planes(quarter + 1, far - 1)

    def whole(buffer, sem, count):
        view = buffer.at[pl.ds(0, count)]
        return pltpu.make_async_copy(view, view, sem)

    def pass_rows():
        whole(relay_rows, relay_in, len(crossing) * 2 * CAP).wait()
        for way, dz, dxl in crossing:
            place = (n_z - 1) * plane + dxl * CORES + way
            pltpu.make_async_remote_copy(
                src_ref=relay_rows.at[pl.ds((way * X_LO + dxl) * 2 * CAP, 2 * CAP)],
                dst_ref=recv.at[pl.ds(place * 2 * CAP, 2 * CAP)],
                send_sem=relay_out,
                recv_sem=a2a_recv.at[1],
                device_id=(me_o, rep_at(dz, dxl, way)),
                device_id_type=MESH,
            ).start()

    def pass_back():
        whole(relay_back, relay_back_in, len(crossing) * CAP).wait()
        for way, dz, dxl in crossing:
            pltpu.make_async_remote_copy(
                src_ref=relay_back.at[pl.ds((way * X_LO + dxl) * CAP, CAP)],
                dst_ref=returned.at[pl.ds(rep_at(-dz, 0, 0) * CAP, CAP)],
                send_sem=relay_back_out,
                recv_sem=ret_recv,
                device_id=(me_o, rep_at(dz, dxl, way)),
                device_id_type=MESH,
            ).start()

    partner_copy.wait()
    for way in (0, 1):
        if (way, 0, True) in ring_hops(0):
            ring_copy(way, 0, True).start()
    for s in range(half):
        for way, s_, other in ring_hops(s):
            ring_copy(way, s, other).wait_recv()
            if s + 1 < half and (way, s + 1, other) in ring_hops(s + 1):
                ring_copy(way, s + 1, other).start()
        if s == half // 2 - 1:
            pass_rows()

    def forward(g):
        def widen(r, carry):
            block = recv[pl.ds((g * group + r) * 2 * CAP, 2 * CAP)].astype(jnp.float32)
            for c in range(CAP):
                at = pl.ds(pl.multiple_of((r * CAP + c) * n_own, n_own), n_own)
                wide[0, at, :] = block[c]
                wide[1, at, :] = block[CAP + c]
            return carry

        lax.fori_loop(0, group, widen, 0)
        mine = pl.ds(g * rows, rows)
        gate = jnp.zeros((rows, hw), jnp.float32)
        up = jnp.zeros_like(gate)
        grad_back = jnp.zeros_like(gate)
        for p in range(n_y):
            pair = []
            for i, kept in enumerate((xs, dys)):
                parts = []
                for h in range(X_HI):
                    j = X_HI * p + h
                    part = wide[i, pl.ds(j, rows, stride=n_own), :].astype(jnp.bfloat16)
                    kept[j, mine, :] = part
                    parts.append(part)
                pair.append(jnp.concatenate(parts, axis=1))
            w_of = [
                jnp.concatenate([weights[X_HI * p + h, k] for h in range(X_HI)], axis=0)
                for k in range(3)
            ]
            gate += nn(pair[0], w_of[0])
            up += nn(pair[0], w_of[1])
            grad_back += nn(pair[1], w_of[2])
        sg = jax.nn.sigmoid(gate)
        silu = gate * sg
        hidden_s[mine, :] = (silu * up).astype(jnp.bfloat16)
        grads_h[mine, :hw] = (grad_back * up * sg * (1.0 + gate * (1.0 - sg))).astype(jnp.bfloat16)
        grads_h[mine, hw:] = (grad_back * silu).astype(jnp.bfloat16)

    def give_back(g):
        mine = pl.ds(g * rows, rows)
        for j in range(n_own):
            wide[0, pl.ds(j, rows, stride=n_own), :] = nt(
                grads_h[mine, :hw], weights[j, 0]
            ) + nt(grads_h[mine, hw:], weights[j, 1])

        def narrow(r, carry):
            for c in range(CAP):
                at = pl.ds(pl.multiple_of((r * CAP + c) * n_own, n_own), n_own)
                back[g * rows + r * CAP + c] = wide[0, at, :].astype(jnp.bfloat16)
            return carry

        lax.fori_loop(0, group, narrow, 0)

        def home(at, dz, members):
            for dxl, dc in members:
                place = at * plane + dxl * CORES + dc
                pltpu.make_async_remote_copy(
                    src_ref=back.at[pl.ds(place * CAP, CAP)],
                    dst_ref=returned.at[pl.ds(me_r * CAP, CAP)],
                    send_sem=ret_send,
                    recv_sem=ret_recv,
                    device_id=(me_o, rep_at(dz, dxl, dc)),
                    device_id_type=MESH,
                ).start()

        def homes(at, carry):
            up_z = (at + 1) // 2
            home(at, jnp.where(lax.rem(at, 2) == 1, up_z, -up_z), in_plane)
            return carry

        if g == 0:
            home(0, 0, in_plane[1:])
            lax.fori_loop(1, far, homes, 0)
            return
        for way, dz, dxl in crossing:
            place = (n_z - 1) * plane + dxl * CORES + way
            via(
                back.at[pl.ds(place * CAP, CAP)],
                relay_back.at[pl.ds((way * X_LO + dxl) * CAP, CAP)],
                ret_send,
                relay_back_in,
                dz,
            )
        lax.fori_loop(far, n_z - 1, homes, 0)

    self_copy.wait()
    whole(recv, a2a_recv.at[0], (group - 1) * 2 * CAP).wait()
    forward(0)
    give_back(0)
    back_copy = pltpu.make_async_copy(
        back.at[pl.ds(0, CAP)], returned.at[pl.ds(me_r * CAP, CAP)], local_sem.at[0]
    )
    back_copy.start()
    whole(recv, a2a_recv.at[1], group * 2 * CAP).wait()
    forward(1)

    def terms(dy, column):
        j = own_at(dy, xh if column else 1 - xh)
        both = tn(xs[j], grads_h[...])
        return both[:, :hw], both[:, hw:], tn(dys[j], hidden_s[...])

    def sum_copy(way, s, column):
        return pltpu.make_async_remote_copy(
            src_ref=stage.at[way, s, column],
            dst_ref=chain.at[way, s, column],
            send_sem=rs_send.at[way, s, column],
            recv_sem=rs_recv.at[way, s, column],
            device_id=towards[way],
            device_id_type=MESH,
        )

    def columns(way, s):
        return range(X_HI) if s > 0 else (way,)

    def put_terms(s):
        for column in range(X_HI):
            for way in (0, 1):
                if column in columns(way, s):
                    distance = half - s
                    for k, term in enumerate(terms(distance if way == 0 else -distance, column)):
                        stage[way, s, column, k] = term.astype(jnp.bfloat16)

    put_terms(0)
    for way in (0, 1):
        sum_copy(way, 0, way).start()
    give_back(1)
    for s in range(1, half):
        put_terms(s)
        for column in range(X_HI):
            for way in (0, 1):
                if column in columns(way, s - 1):
                    sum_copy(way, s - 1, column).wait_recv()
                    for k in range(3):
                        stage[way, s, column, k] = (
                            stage[way, s, column, k].astype(jnp.float32)
                            + chain[way, s - 1, column, k].astype(jnp.float32)
                        ).astype(jnp.bfloat16)
                sum_copy(way, s, column).start()
        if s == min(2, half - 1):
            pass_back()
    for column in range(X_HI):
        for k, term in enumerate(terms(0, column)):
            total[column, k] = term.astype(jnp.bfloat16).astype(jnp.float32)

    def summed(column, k):
        return (
            total[column, k]
            + chain[0, half - 1, column, k].astype(jnp.float32)
            + chain[1, half - 1, column, k].astype(jnp.float32)
        )

    for way in (0, 1):
        sum_copy(way, half - 1, 0).wait_recv()
    for k in range(3):
        cross[k] = summed(0, k).astype(jnp.bfloat16)
    cross_copy = pltpu.make_async_remote_copy(
        src_ref=cross,
        dst_ref=crossed,
        send_sem=rsx_send,
        recv_sem=rsx_recv,
        device_id=partner,
        device_id_type=MESH,
    )
    cross_copy.start()
    for way in (0, 1):
        sum_copy(way, half - 1, 1).wait_recv()
    for k in range(3):
        total[1, k] = summed(1, k)

    back_copy.wait()
    whole(returned, ret_recv, (n_rep - 1) * CAP).wait()

    def pick(t, carry):
        xg_ref[t] = returned[pos_ref[t]]
        return carry

    lax.fori_loop(0, toks, pick, 0)

    cross_copy.wait()
    for k in range(3):
        sums_ref[k] = total[1, k] + crossed[k].astype(jnp.float32)

    whole(send, a2a_send, (n_rep - 1) * 2 * CAP).wait()
    whole(back, ret_send, (n_rep - 1) * CAP).wait()
    whole(relay_rows, relay_out, len(crossing) * 2 * CAP).wait()
    whole(relay_back, relay_back_out, len(crossing) * CAP).wait()
    for s in range(half):
        for way, s_, other in ring_hops(s):
            ring_copy(way, s, other).wait_send()
        for way in (0, 1):
            for column in columns(way, s):
                sum_copy(way, s, column).wait_send()


def shards(n_own, n_rep, tokens, cotangent, route, host, w_gate, w_up, w_down_t):
    tok_rows, width = tokens.shape
    hw = w_gate.shape[2]
    piece = w_gate.shape[1]
    lanes = width // n_own
    rows = n_rep * CAP
    labels = lax.broadcasted_iota(jnp.int32, (tok_rows, n_rep), 1)
    target = jnp.sum(jnp.where(route == labels, host[None, :], 0), axis=1)
    earlier = lax.broadcasted_iota(jnp.int32, (tok_rows, tok_rows), 1) < lax.broadcasted_iota(
        jnp.int32, (tok_rows, tok_rows), 0
    )
    arrival = jnp.sum(
        jnp.where((target[:, None] == target[None, :]) & earlier, 1, 0), axis=1
    )
    position = target * CAP + arrival
    slot_ids = lax.broadcasted_iota(jnp.int32, (rows, tok_rows), 0)
    token_ids = lax.broadcasted_iota(jnp.int32, (rows, tok_rows), 1)
    source = tok_rows + jnp.sum(
        jnp.where(slot_ids == position[None, :], token_ids - tok_rows, 0), axis=1
    )
    bf16, f32 = jnp.bfloat16, jnp.float32
    half = n_own // X_HI // 2
    vmem = pl.BlockSpec(memory_space=pltpu.VMEM)
    smem = pl.BlockSpec(memory_space=pltpu.SMEM)
    anywhere = pl.BlockSpec(memory_space=pl.ANY)
    dma = pltpu.SemaphoreType.DMA
    x_rows, sums = pl.pallas_call(
        functools.partial(kernel, n_own, n_rep),
        out_shape=(
            jax.ShapeDtypeStruct((tok_rows, n_own, lanes), bf16),
            jax.ShapeDtypeStruct((3, piece, hw), f32),
        ),
        in_specs=[smem, smem] + [anywhere] * 5,
        out_specs=(vmem,) * 2,
        scratch_shapes=[
            pltpu.VMEM((2, tok_rows, width), bf16),
            pltpu.VMEM((tok_rows + 1, n_own, lanes), bf16),
            pltpu.VMEM((tok_rows + 1, n_own, lanes), bf16),
            pltpu.VMEM((2 * rows, n_own, lanes), bf16),
            pltpu.VMEM((2 * rows, n_own, lanes), bf16),
            pltpu.VMEM((n_own, 3, piece, hw), bf16),
            pltpu.VMEM((2, max(rows // 2, tok_rows) * n_own, lanes), f32),
            pltpu.VMEM((n_own, rows, lanes), bf16),
            pltpu.VMEM((n_own, rows, lanes), bf16),
            pltpu.VMEM((rows, 2 * hw), bf16),
            pltpu.VMEM((rows, hw), bf16),
            pltpu.VMEM((rows, n_own, lanes), bf16),
            pltpu.VMEM((rows, n_own, lanes), bf16),
            pltpu.VMEM((2, half, X_HI, 3, piece, hw), bf16),
            pltpu.VMEM((2, half, X_HI, 3, piece, hw), bf16),
            pltpu.VMEM((X_HI, 3, piece, hw), f32),
            pltpu.VMEM((3, piece, hw), bf16),
            pltpu.VMEM((3, piece, hw), bf16),
            pltpu.VMEM((4 * CAP * X_LO, n_own, lanes), bf16),
            pltpu.VMEM((2 * CAP * X_LO, n_own, lanes), bf16),
            dma((5,)),
            pltpu.SemaphoreType.REGULAR((2, n_rep // (X_LO * CORES) // 2 - 1)),
            dma,
            dma,
            dma,
            dma,
            dma,
            dma((2,)),
            dma,
            dma,
            dma,
            dma,
            dma((2, half, 2)),
            dma((2, half, 2)),
            dma((2, half, 2)),
            dma((2, half, 2)),
            dma,
            dma,
        ],
        compiler_params=pltpu.CompilerParams(collective_id=0, has_side_effects=True),
    )(source, position, tokens, cotangent, w_gate, w_up, w_down_t)
    return (x_rows.reshape(tok_rows, width), sums[0:1], sums[1:2], sums[2:3])


def solution(mesh):
    body = functools.partial(shards, mesh.shape["own"], mesh.shape["rep"])
    return jax.shard_map(
        body,
        mesh=mesh,
        in_specs=(
            P(("own", "rep"), None),
            P(("own", "rep"), None),
            P(("own", "rep"), None),
            P(),
            P("rep", "own", None),
            P("rep", "own", None),
            P("rep", "own", None),
        ),
        out_specs=(
            P(("own", "rep"), None),
            P("rep", "own", None),
            P("rep", "own", None),
            P("rep", "own", None),
        ),
        check_vma=False,
    )
```

```python
import functools

import jax
import jax.numpy as jnp
from jax import lax
from jax.experimental import pallas as pl
from jax.experimental.pallas import tpu as pltpu
from jax.sharding import PartitionSpec as P

MESH = pl.DeviceIdType.MESH
CAP = 3
CORES = 2
X_LO = 2
X_HI = 2


def nn(left, right):
    return lax.dot_general(
        left, right, (((1,), (0,)), ((), ())), preferred_element_type=jnp.float32
    )


def nt(left, right):
    return lax.dot_general(
        left, right, (((1,), (1,)), ((), ())), preferred_element_type=jnp.float32
    )


def tn(left, right):
    return lax.dot_general(
        left, right, (((0,), (0,)), ((), ())), preferred_element_type=jnp.float32
    )


def kernel(
    n_own,
    n_rep,
    route_ref,
    host_ref,
    tok_ref,
    cot_ref,
    wg_ref,
    wu_ref,
    wd_ref,
    xg_ref,
    sums_ref,
    route_in,
    host_in,
    table,
    index,
    tok_in,
    x_of,
    dy_of,
    send,
    recv,
    weights,
    wide,
    xs,
    dys,
    grads_h,
    hidden_s,
    back,
    returned,
    stage,
    chain,
    total,
    cross,
    crossed,
    relay_rows,
    relay_back,
    local_sem,
    ready,
    relay_in,
    relay_out,
    relay_back_in,
    relay_back_out,
    a2a_send,
    a2a_recv,
    ret_send,
    ret_recv,
    agx_send,
    agx_recv,
    ag_send,
    ag_recv,
    rs_send,
    rs_recv,
    rsx_send,
    rsx_recv,
):
    n_y = n_own // X_HI
    n_z = n_rep // (X_LO * CORES)
    half = n_y // 2
    plane = X_LO * CORES
    far = n_z // 2
    quarter = n_z // 4
    group = n_rep // 2
    rows = group * CAP
    hw = wg_ref.shape[2]
    toks = tok_ref.shape[0]
    lanes = tok_ref.shape[1] // n_own
    me_o = lax.axis_index("own")
    me_r = lax.axis_index("rep")
    y = me_o // X_HI
    xh = lax.rem(me_o, X_HI)
    xl = me_r // (n_z * CORES)
    z = lax.rem(me_r // CORES, n_z)
    core = lax.rem(me_r, CORES)

    def own_at(dy, h):
        return lax.rem(y + dy + n_y, n_y) * X_HI + h

    right = (own_at(1, xh), me_r)
    left = (own_at(-1, xh), me_r)
    partner = (y * X_HI + (1 - xh), me_r)
    towards = (right, left)

    def rep_at(dz, dxl, dc):
        return (
            lax.rem(xl + dxl, X_LO) * (n_z * CORES)
            + lax.rem(z + dz + n_z, n_z) * CORES
            + lax.rem(core + dc, CORES)
        )

    def signal(sem, dev):
        pl.semaphore_signal(sem, inc=1, device_id=dev, device_id_type=MESH)

    in_plane = [(dxl, dc) for dxl in range(X_LO) for dc in range(CORES)]
    ahead = (me_o, rep_at(1, 0, 0))
    behind = (me_o, rep_at(-1, 0, 0))
    barrier = pltpu.get_barrier_semaphore()
    for dev in (right, left, partner, ahead, behind):
        signal(barrier, dev)
    for dxl, dc in in_plane[1:]:
        signal(barrier, (me_o, rep_at(0, dxl, dc)))

    names = [
        pltpu.make_async_copy(route_ref, route_in, local_sem.at[5]),
        pltpu.make_async_copy(host_ref, host_in, local_sem.at[6]),
    ]
    loads = [
        pltpu.make_async_copy(ref, tok_in.at[i], local_sem.at[3 + i])
        for i, ref in enumerate((tok_ref, cot_ref))
    ] + [
        pltpu.make_async_copy(w_ref.at[0], weights.at[me_o, k], local_sem.at[k])
        for k, w_ref in enumerate((wg_ref, wu_ref, wd_ref))
    ]
    for copy in names + loads:
        copy.start()

    for copy in names:
        copy.wait()
    def across(shape, axis):
        return lax.broadcasted_iota(jnp.int32, shape, axis)

    def turned(row, size):
        eye = across((size, row.shape[1]), 0) == across((size, row.shape[1]), 1)
        return jnp.sum(jnp.where(eye, row, 0), axis=1, keepdims=True)

    route_row = route_in[...]
    host_col = turned(host_in[...], n_rep)
    named = across((n_rep, toks), 0) == route_row
    target_row = jnp.sum(jnp.where(named, host_col, 0), axis=0, keepdims=True)
    square = (toks, toks)
    same = (turned(target_row, toks) == target_row) & (across(square, 0) < across(square, 1))
    arrival_row = jnp.sum(jnp.where(same, 1, 0), axis=0, keepdims=True)
    position_row = target_row * CAP + arrival_row
    slots = index.shape[1]
    spread = (toks, slots)
    holds = turned(position_row, toks) == across(spread, 1)
    source_row = toks + jnp.sum(
        jnp.where(holds, across(spread, 0) - toks, 0), axis=0, keepdims=True
    )
    table[0:1, :] = source_row
    table[1:2, 0:toks] = position_row
    to_scalars = pltpu.make_async_copy(table, index, local_sem.at[5])
    to_scalars.start()

    for i in range(2):
        loads[i].wait()
        for j in range(n_own):
            wide[i, pl.ds(j, toks, stride=n_own), :] = tok_in[
                i, :, j * lanes : (j + 1) * lanes
            ].astype(jnp.float32)

    def by_token(t, carry):
        at = pl.ds(pl.multiple_of(t * n_own, n_own), n_own)
        x_of[t] = wide[0, at, :].astype(jnp.bfloat16)
        dy_of[t] = wide[1, at, :].astype(jnp.bfloat16)
        return carry

    lax.fori_loop(0, toks, by_token, 0, unroll=4)
    for rows_of in (x_of, dy_of):
        rows_of[toks] = jnp.zeros((n_own, lanes), jnp.bfloat16)

    def fill_plane(dz):
        for dxl, dc in in_plane:
            r = rep_at(dz, dxl, dc)
            for c in range(CAP):
                row = jnp.clip(index[0, r * CAP + c], 0, toks)
                send[r * 2 * CAP + c] = x_of[row]
                send[r * 2 * CAP + CAP + c] = dy_of[row]

    def fill_both(d):
        fill_plane(d)
        fill_plane(-d)

    to_scalars.wait()
    fill_plane(0)
    fill_both(1)
    for copy in loads[2:]:
        copy.wait()
    pl.semaphore_wait(barrier, 5 + plane - 1)

    signal(ready.at[0, 0], ahead)
    signal(ready.at[1, 0], behind)

    def weight_copy(block, dev, s_sem, r_sem):
        return pltpu.make_async_remote_copy(
            src_ref=weights.at[block],
            dst_ref=weights.at[block],
            send_sem=s_sem,
            recv_sem=r_sem,
            device_id=dev,
            device_id_type=MESH,
        )

    partner_copy = weight_copy(me_o, partner, agx_send, agx_recv)
    partner_copy.start()

    def ring_copy(way, s, other):
        h = (1 - xh) if other else xh
        block = own_at(-s if way == 0 else s, h)
        return weight_copy(
            block,
            towards[way],
            ag_send.at[way, s, int(other)],
            ag_recv.at[way, s, int(other)],
        )

    def ring_hops(s):
        if s < half - 1:
            return [(way, s, other) for other in (False, True) for way in (0, 1)]
        return [(0, s, False), (1, s, True)]

    for way in (0, 1):
        if (way, 0, False) in ring_hops(0):
            ring_copy(way, 0, False).start()

    def send_plane(dz, at, members):
        for dxl, dc in members:
            r = rep_at(dz, dxl, dc)
            place = at * plane + dxl * CORES + dc
            pltpu.make_async_remote_copy(
                src_ref=send.at[pl.ds(r * 2 * CAP, 2 * CAP)],
                dst_ref=recv.at[pl.ds(place * 2 * CAP, 2 * CAP)],
                send_sem=a2a_send,
                recv_sem=a2a_recv.at[at // far],
                device_id=(me_o, r),
                device_id_type=MESH,
            ).start()

    send_plane(0, 0, in_plane[1:])
    self_copy = pltpu.make_async_copy(
        send.at[pl.ds(me_r * 2 * CAP, 2 * CAP)],
        recv.at[pl.ds(0, 2 * CAP)],
        local_sem.at[0],
    )
    self_copy.start()

    def send_both(d, forward):
        for way, ahead_of in enumerate((ahead, behind)):
            pl.semaphore_wait(ready.at[way, d - 1], 1)
            if forward:
                signal(ready.at[way, d], ahead_of)
        send_plane(d, 2 * d, in_plane)
        send_plane(-d, 2 * d - 1, in_plane)
        if forward:
            fill_both(d + 1)

    def send_planes(first, last):
        def one(d, carry):
            send_both(d, True)
            return carry

        lax.fori_loop(first, min(last + 1, far - 1), one, 0)
        if last == far - 1:
            send_both(last, False)

    ways = [(0, quarter), (1, -quarter)]
    crossing = [(way, dz, dxl) for way, dz in ways for dxl in range(X_LO)]

    def via(src, dst, s_sem, r_sem, dz):
        pltpu.make_async_remote_copy(
            src_ref=src,
            dst_ref=dst,
            send_sem=s_sem,
            recv_sem=r_sem,
            device_id=(me_o, rep_at(dz, 0, 0)),
            device_id_type=MESH,
        ).start()

    fill_plane(far)
    send_planes(1, quarter)
    for way, dz, dxl in crossing:
        r = rep_at(far, dxl, way)
        via(
            send.at[pl.ds(r * 2 * CAP, 2 * CAP)],
            relay_rows.at[pl.ds((way * X_LO + dxl) * 2 * CAP, 2 * CAP)],
            a2a_send,
            relay_in,
            dz,
        )
    if quarter < far - 1:
        send_planes(quarter + 1, far - 1)

    def whole(buffer, sem, count):
        view = buffer.at[pl.ds(0, count)]
        return pltpu.make_async_copy(view, view, sem)

    def pass_rows():
        whole(relay_rows, relay_in, len(crossing) * 2 * CAP).wait()
        for way, dz, dxl in crossing:
            place = (n_z - 1) * plane + dxl * CORES + way
            pltpu.make_async_remote_copy(
                src_ref=relay_rows.at[pl.ds((way * X_LO + dxl) * 2 * CAP, 2 * CAP)],
                dst_ref=recv.at[pl.ds(place * 2 * CAP, 2 * CAP)],
                send_sem=relay_out,
                recv_sem=a2a_recv.at[1],
                device_id=(me_o, rep_at(dz, dxl, way)),
                device_id_type=MESH,
            ).start()

    def pass_back():
        whole(relay_back, relay_back_in, len(crossing) * CAP).wait()
        for way, dz, dxl in crossing:
            pltpu.make_async_remote_copy(
                src_ref=relay_back.at[pl.ds((way * X_LO + dxl) * CAP, CAP)],
                dst_ref=returned.at[pl.ds(rep_at(-dz, 0, 0) * CAP, CAP)],
                send_sem=relay_back_out,
                recv_sem=ret_recv,
                device_id=(me_o, rep_at(dz, dxl, way)),
                device_id_type=MESH,
            ).start()

    partner_copy.wait()
    for way in (0, 1):
        if (way, 0, True) in ring_hops(0):
            ring_copy(way, 0, True).start()
    for s in range(half):
        for way, s_, other in ring_hops(s):
            ring_copy(way, s, other).wait_recv()
            if s + 1 < half and (way, s + 1, other) in ring_hops(s + 1):
                ring_copy(way, s + 1, other).start()
        if s == half // 2 - 1:
            pass_rows()

    def forward(g):
        def widen(r, carry):
            block = recv[pl.ds((g * group + r) * 2 * CAP, 2 * CAP)].astype(jnp.float32)
            for c in range(CAP):
                at = pl.ds(pl.multiple_of((r * CAP + c) * n_own, n_own), n_own)
                wide[0, at, :] = block[c]
                wide[1, at, :] = block[CAP + c]
            return carry

        lax.fori_loop(0, group, widen, 0)
        mine = pl.ds(g * rows, rows)
        gate = jnp.zeros((rows, hw), jnp.float32)
        up = jnp.zeros_like(gate)
        grad_back = jnp.zeros_like(gate)
        for p in range(n_y):
            pair = []
            for i, kept in enumerate((xs, dys)):
                parts = []
                for h in range(X_HI):
                    j = X_HI * p + h
                    part = wide[i, pl.ds(j, rows, stride=n_own), :].astype(jnp.bfloat16)
                    kept[j, mine, :] = part
                    parts.append(part)
                pair.append(jnp.concatenate(parts, axis=1))
            w_of = [
                jnp.concatenate([weights[X_HI * p + h, k] for h in range(X_HI)], axis=0)
                for k in range(3)
            ]
            gate += nn(pair[0], w_of[0])
            up += nn(pair[0], w_of[1])
            grad_back += nn(pair[1], w_of[2])
        sg = jax.nn.sigmoid(gate)
        silu = gate * sg
        hidden_s[mine, :] = (silu * up).astype(jnp.bfloat16)
        grads_h[mine, :hw] = (grad_back * up * sg * (1.0 + gate * (1.0 - sg))).astype(jnp.bfloat16)
        grads_h[mine, hw:] = (grad_back * silu).astype(jnp.bfloat16)

    def give_back(g):
        mine = pl.ds(g * rows, rows)
        for j in range(n_own):
            wide[0, pl.ds(j, rows, stride=n_own), :] = nt(
                grads_h[mine, :hw], weights[j, 0]
            ) + nt(grads_h[mine, hw:], weights[j, 1])

        def narrow(r, carry):
            for c in range(CAP):
                at = pl.ds(pl.multiple_of((r * CAP + c) * n_own, n_own), n_own)
                back[g * rows + r * CAP + c] = wide[0, at, :].astype(jnp.bfloat16)
            return carry

        lax.fori_loop(0, group, narrow, 0)

        def home(at, dz, members):
            for dxl, dc in members:
                place = at * plane + dxl * CORES + dc
                pltpu.make_async_remote_copy(
                    src_ref=back.at[pl.ds(place * CAP, CAP)],
                    dst_ref=returned.at[pl.ds(me_r * CAP, CAP)],
                    send_sem=ret_send,
                    recv_sem=ret_recv,
                    device_id=(me_o, rep_at(dz, dxl, dc)),
                    device_id_type=MESH,
                ).start()

        def homes(at, carry):
            up_z = (at + 1) // 2
            home(at, jnp.where(lax.rem(at, 2) == 1, up_z, -up_z), in_plane)
            return carry

        if g == 0:
            home(0, 0, in_plane[1:])
            lax.fori_loop(1, far, homes, 0)
            return
        for way, dz, dxl in crossing:
            place = (n_z - 1) * plane + dxl * CORES + way
            via(
                back.at[pl.ds(place * CAP, CAP)],
                relay_back.at[pl.ds((way * X_LO + dxl) * CAP, CAP)],
                ret_send,
                relay_back_in,
                dz,
            )
        lax.fori_loop(far, n_z - 1, homes, 0)

    self_copy.wait()
    whole(recv, a2a_recv.at[0], (group - 1) * 2 * CAP).wait()
    forward(0)
    give_back(0)
    back_copy = pltpu.make_async_copy(
        back.at[pl.ds(0, CAP)], returned.at[pl.ds(me_r * CAP, CAP)], local_sem.at[0]
    )
    back_copy.start()
    whole(recv, a2a_recv.at[1], group * 2 * CAP).wait()
    forward(1)

    def terms(dy, column):
        j = own_at(dy, xh if column else 1 - xh)
        both = tn(xs[j], grads_h[...])
        return both[:, :hw], both[:, hw:], tn(dys[j], hidden_s[...])

    def sum_copy(way, s, column):
        return pltpu.make_async_remote_copy(
            src_ref=stage.at[way, s, column],
            dst_ref=chain.at[way, s, column],
            send_sem=rs_send.at[way, s, column],
            recv_sem=rs_recv.at[way, s, column],
            device_id=towards[way],
            device_id_type=MESH,
        )

    def columns(way, s):
        return range(X_HI) if s > 0 else (way,)

    def put_terms(s):
        for column in range(X_HI):
            for way in (0, 1):
                if column in columns(way, s):
                    distance = half - s
                    for k, term in enumerate(terms(distance if way == 0 else -distance, column)):
                        stage[way, s, column, k] = term.astype(jnp.bfloat16)

    put_terms(0)
    for way in (0, 1):
        sum_copy(way, 0, way).start()
    give_back(1)
    for s in range(1, half):
        put_terms(s)
        for column in range(X_HI):
            for way in (0, 1):
                if column in columns(way, s - 1):
                    sum_copy(way, s - 1, column).wait_recv()
                    for k in range(3):
                        stage[way, s, column, k] = (
                            stage[way, s, column, k].astype(jnp.float32)
                            + chain[way, s - 1, column, k].astype(jnp.float32)
                        ).astype(jnp.bfloat16)
                sum_copy(way, s, column).start()
        if s == min(2, half - 1):
            pass_back()
    for column in range(X_HI):
        for k, term in enumerate(terms(0, column)):
            total[column, k] = term.astype(jnp.bfloat16).astype(jnp.float32)

    def summed(column, k):
        return (
            total[column, k]
            + chain[0, half - 1, column, k].astype(jnp.float32)
            + chain[1, half - 1, column, k].astype(jnp.float32)
        )

    for way in (0, 1):
        sum_copy(way, half - 1, 0).wait_recv()
    for k in range(3):
        cross[k] = summed(0, k).astype(jnp.bfloat16)
    cross_copy = pltpu.make_async_remote_copy(
        src_ref=cross,
        dst_ref=crossed,
        send_sem=rsx_send,
        recv_sem=rsx_recv,
        device_id=partner,
        device_id_type=MESH,
    )
    cross_copy.start()
    for way in (0, 1):
        sum_copy(way, half - 1, 1).wait_recv()
    for k in range(3):
        total[1, k] = summed(1, k)

    back_copy.wait()
    whole(returned, ret_recv, (n_rep - 1) * CAP).wait()

    def pick(t, carry):
        xg_ref[t] = returned[jnp.clip(index[1, t], 0, n_rep * CAP - 1)]
        return carry

    lax.fori_loop(0, toks, pick, 0)

    cross_copy.wait()
    for k in range(3):
        sums_ref[k] = total[1, k] + crossed[k].astype(jnp.float32)

    whole(send, a2a_send, (n_rep - 1) * 2 * CAP).wait()
    whole(back, ret_send, (n_rep - 1) * CAP).wait()
    whole(relay_rows, relay_out, len(crossing) * 2 * CAP).wait()
    whole(relay_back, relay_back_out, len(crossing) * CAP).wait()
    for s in range(half):
        for way, s_, other in ring_hops(s):
            ring_copy(way, s, other).wait_send()
        for way in (0, 1):
            for column in columns(way, s):
                sum_copy(way, s, column).wait_send()


def shards(n_own, n_rep, tokens, cotangent, route, host, w_gate, w_up, w_down_t):
    tok_rows, width = tokens.shape
    hw = w_gate.shape[2]
    piece = w_gate.shape[1]
    lanes = width // n_own
    rows = n_rep * CAP
    bf16, f32 = jnp.bfloat16, jnp.float32
    half = n_own // X_HI // 2
    vmem = pl.BlockSpec(memory_space=pltpu.VMEM)
    table = (2, -(-max(rows, tok_rows) // 128) * 128)
    anywhere = pl.BlockSpec(memory_space=pl.ANY)
    dma = pltpu.SemaphoreType.DMA
    x_rows, sums = pl.pallas_call(
        functools.partial(kernel, n_own, n_rep),
        out_shape=(
            jax.ShapeDtypeStruct((tok_rows, n_own, lanes), bf16),
            jax.ShapeDtypeStruct((3, piece, hw), f32),
        ),
        in_specs=[anywhere] * 7,
        out_specs=(vmem,) * 2,
        scratch_shapes=[
            pltpu.VMEM((1, tok_rows), jnp.int32),
            pltpu.VMEM((1, n_rep), jnp.int32),
            pltpu.VMEM(table, jnp.int32),
            pltpu.SMEM(table, jnp.int32),
            pltpu.VMEM((2, tok_rows, width), bf16),
            pltpu.VMEM((tok_rows + 1, n_own, lanes), bf16),
            pltpu.VMEM((tok_rows + 1, n_own, lanes), bf16),
            pltpu.VMEM((2 * rows, n_own, lanes), bf16),
            pltpu.VMEM((2 * rows, n_own, lanes), bf16),
            pltpu.VMEM((n_own, 3, piece, hw), bf16),
            pltpu.VMEM((2, max(rows // 2, tok_rows) * n_own, lanes), f32),
            pltpu.VMEM((n_own, rows, lanes), bf16),
            pltpu.VMEM((n_own, rows, lanes), bf16),
            pltpu.VMEM((rows, 2 * hw), bf16),
            pltpu.VMEM((rows, hw), bf16),
            pltpu.VMEM((rows, n_own, lanes), bf16),
            pltpu.VMEM((rows, n_own, lanes), bf16),
            pltpu.VMEM((2, half, X_HI, 3, piece, hw), bf16),
            pltpu.VMEM((2, half, X_HI, 3, piece, hw), bf16),
            pltpu.VMEM((X_HI, 3, piece, hw), f32),
            pltpu.VMEM((3, piece, hw), bf16),
            pltpu.VMEM((3, piece, hw), bf16),
            pltpu.VMEM((4 * CAP * X_LO, n_own, lanes), bf16),
            pltpu.VMEM((2 * CAP * X_LO, n_own, lanes), bf16),
            dma((7,)),
            pltpu.SemaphoreType.REGULAR((2, n_rep // (X_LO * CORES) // 2 - 1)),
            dma,
            dma,
            dma,
            dma,
            dma,
            dma((2,)),
            dma,
            dma,
            dma,
            dma,
            dma((2, half, 2)),
            dma((2, half, 2)),
            dma((2, half, 2)),
            dma((2, half, 2)),
            dma,
            dma,
        ],
        compiler_params=pltpu.CompilerParams(collective_id=0, has_side_effects=True),
    )(route.reshape(1, tok_rows), host[None], tokens, cotangent, w_gate, w_up, w_down_t)
    return (x_rows.reshape(tok_rows, width), sums[0:1], sums[1:2], sums[2:3])


def solution(mesh):
    body = functools.partial(shards, mesh.shape["own"], mesh.shape["rep"])
    return jax.shard_map(
        body,
        mesh=mesh,
        in_specs=(
            P(("own", "rep"), None),
            P(("own", "rep"), None),
            P(("own", "rep"), None),
            P(),
            P("rep", "own", None),
            P("rep", "own", None),
            P("rep", "own", None),
        ),
        out_specs=(
            P(("own", "rep"), None),
            P("rep", "own", None),
            P("rep", "own", None),
            P("rep", "own", None),
        ),
        check_vma=False,
    )
```

```python
import functools

import jax
import jax.numpy as jnp
from jax import lax
from jax.experimental import pallas as pl
from jax.experimental.pallas import tpu as pltpu
from jax.sharding import PartitionSpec as P

MESH = pl.DeviceIdType.MESH
CAP = 3
CORES = 2
X_LO = 2
X_HI = 2


def nn(left, right):
    return lax.dot_general(
        left, right, (((1,), (0,)), ((), ())), preferred_element_type=jnp.float32
    )


def nt(left, right):
    return lax.dot_general(
        left, right, (((1,), (1,)), ((), ())), preferred_element_type=jnp.float32
    )


def tn(left, right):
    return lax.dot_general(
        left, right, (((0,), (0,)), ((), ())), preferred_element_type=jnp.float32
    )


def kernel(
    n_own,
    n_rep,
    route_ref,
    host_ref,
    tok_ref,
    cot_ref,
    wg_ref,
    wu_ref,
    wd_ref,
    xg_ref,
    sums_ref,
    route_in,
    host_in,
    table,
    index,
    tok_in,
    x_of,
    dy_of,
    send,
    recv,
    weights,
    wide,
    xs,
    dys,
    grads_h,
    hidden_s,
    back,
    returned,
    stage,
    chain,
    total,
    cross,
    crossed,
    early,
    earlier,
    relay_rows,
    relay_back,
    local_sem,
    ready,
    relay_in,
    relay_out,
    relay_back_in,
    relay_back_out,
    a2a_send,
    a2a_recv,
    ret_send,
    ret_recv,
    agx_send,
    agx_recv,
    ag_send,
    ag_recv,
    rs_send,
    rs_recv,
    rsx_send,
    rsx_recv,
    first_send,
    first_recv,
):
    n_y = n_own // X_HI
    n_z = n_rep // (X_LO * CORES)
    half = n_y // 2
    plane = X_LO * CORES
    far = n_z // 2
    quarter = n_z // 4
    group = n_rep // 2
    rows = group * CAP
    hw = wg_ref.shape[2]
    toks = tok_ref.shape[0]
    lanes = tok_ref.shape[1] // n_own
    me_o = lax.axis_index("own")
    me_r = lax.axis_index("rep")
    y = me_o // X_HI
    xh = lax.rem(me_o, X_HI)
    xl = me_r // (n_z * CORES)
    z = lax.rem(me_r // CORES, n_z)
    core = lax.rem(me_r, CORES)

    def own_at(dy, h):
        return lax.rem(y + dy + n_y, n_y) * X_HI + h

    right = (own_at(1, xh), me_r)
    left = (own_at(-1, xh), me_r)
    partner = (y * X_HI + (1 - xh), me_r)
    towards = (right, left)

    def rep_at(dz, dxl, dc):
        return (
            lax.rem(xl + dxl, X_LO) * (n_z * CORES)
            + lax.rem(z + dz + n_z, n_z) * CORES
            + lax.rem(core + dc, CORES)
        )

    def signal(sem, dev):
        pl.semaphore_signal(sem, inc=1, device_id=dev, device_id_type=MESH)

    in_plane = [(dxl, dc) for dxl in range(X_LO) for dc in range(CORES)]
    ahead = (me_o, rep_at(1, 0, 0))
    behind = (me_o, rep_at(-1, 0, 0))
    barrier = pltpu.get_barrier_semaphore()
    for dev in (right, left, partner, ahead, behind):
        signal(barrier, dev)
    for dxl, dc in in_plane[1:]:
        signal(barrier, (me_o, rep_at(0, dxl, dc)))

    names = [
        pltpu.make_async_copy(route_ref, route_in, local_sem.at[5]),
        pltpu.make_async_copy(host_ref, host_in, local_sem.at[6]),
    ]
    loads = [
        pltpu.make_async_copy(ref, tok_in.at[i], local_sem.at[3 + i])
        for i, ref in enumerate((tok_ref, cot_ref))
    ] + [
        pltpu.make_async_copy(w_ref.at[0], weights.at[me_o, k], local_sem.at[k])
        for k, w_ref in enumerate((wg_ref, wu_ref, wd_ref))
    ]
    for copy in names + loads:
        copy.start()

    for copy in names:
        copy.wait()
    def across(shape, axis):
        return lax.broadcasted_iota(jnp.int32, shape, axis)

    def turned(row, size):
        eye = across((size, row.shape[1]), 0) == across((size, row.shape[1]), 1)
        return jnp.sum(jnp.where(eye, row, 0), axis=1, keepdims=True)

    route_row = route_in[...]
    host_col = turned(host_in[...], n_rep)
    named = across((n_rep, toks), 0) == route_row
    target_row = jnp.sum(jnp.where(named, host_col, 0), axis=0, keepdims=True)
    square = (toks, toks)
    same = (turned(target_row, toks) == target_row) & (across(square, 0) < across(square, 1))
    arrival_row = jnp.sum(jnp.where(same, 1, 0), axis=0, keepdims=True)
    position_row = target_row * CAP + arrival_row
    slots = index.shape[1]
    spread = (toks, slots)
    holds = turned(position_row, toks) == across(spread, 1)
    source_row = toks + jnp.sum(
        jnp.where(holds, across(spread, 0) - toks, 0), axis=0, keepdims=True
    )
    table[0:1, :] = source_row
    table[1:2, 0:toks] = position_row
    to_scalars = pltpu.make_async_copy(table, index, local_sem.at[5])
    to_scalars.start()

    for i in range(2):
        loads[i].wait()
        for j in range(n_own):
            wide[i, pl.ds(j, toks, stride=n_own), :] = tok_in[
                i, :, j * lanes : (j + 1) * lanes
            ].astype(jnp.float32)

    def by_token(t, carry):
        at = pl.ds(pl.multiple_of(t * n_own, n_own), n_own)
        x_of[t] = wide[0, at, :].astype(jnp.bfloat16)
        dy_of[t] = wide[1, at, :].astype(jnp.bfloat16)
        return carry

    lax.fori_loop(0, toks, by_token, 0, unroll=4)
    for rows_of in (x_of, dy_of):
        rows_of[toks] = jnp.zeros((n_own, lanes), jnp.bfloat16)

    def fill_plane(dz):
        for dxl, dc in in_plane:
            r = rep_at(dz, dxl, dc)
            for c in range(CAP):
                row = jnp.clip(index[0, r * CAP + c], 0, toks)
                send[r * 2 * CAP + c] = x_of[row]
                send[r * 2 * CAP + CAP + c] = dy_of[row]

    def fill_both(d):
        fill_plane(d)
        fill_plane(-d)

    to_scalars.wait()
    fill_plane(0)
    fill_both(1)
    for copy in loads[2:]:
        copy.wait()
    pl.semaphore_wait(barrier, 5 + plane - 1)

    signal(ready.at[0, 0], ahead)
    signal(ready.at[1, 0], behind)

    def weight_copy(block, dev, s_sem, r_sem):
        return pltpu.make_async_remote_copy(
            src_ref=weights.at[block],
            dst_ref=weights.at[block],
            send_sem=s_sem,
            recv_sem=r_sem,
            device_id=dev,
            device_id_type=MESH,
        )

    partner_copy = weight_copy(me_o, partner, agx_send, agx_recv)
    partner_copy.start()

    def ring_copy(way, s, other):
        h = (1 - xh) if other else xh
        block = own_at(-s if way == 0 else s, h)
        return weight_copy(
            block,
            towards[way],
            ag_send.at[way, s, int(other)],
            ag_recv.at[way, s, int(other)],
        )

    def ring_hops(s):
        if s < half - 1:
            return [(way, s, other) for other in (False, True) for way in (0, 1)]
        return [(0, s, False), (1, s, True)]

    for way in (0, 1):
        if (way, 0, False) in ring_hops(0):
            ring_copy(way, 0, False).start()

    def send_plane(dz, at, members):
        for dxl, dc in members:
            r = rep_at(dz, dxl, dc)
            place = at * plane + dxl * CORES + dc
            pltpu.make_async_remote_copy(
                src_ref=send.at[pl.ds(r * 2 * CAP, 2 * CAP)],
                dst_ref=recv.at[pl.ds(place * 2 * CAP, 2 * CAP)],
                send_sem=a2a_send,
                recv_sem=a2a_recv.at[at // far],
                device_id=(me_o, r),
                device_id_type=MESH,
            ).start()

    send_plane(0, 0, in_plane[1:])
    self_copy = pltpu.make_async_copy(
        send.at[pl.ds(me_r * 2 * CAP, 2 * CAP)],
        recv.at[pl.ds(0, 2 * CAP)],
        local_sem.at[0],
    )
    self_copy.start()

    def send_both(d, forward):
        for way, ahead_of in enumerate((ahead, behind)):
            pl.semaphore_wait(ready.at[way, d - 1], 1)
            if forward:
                signal(ready.at[way, d], ahead_of)
        send_plane(d, 2 * d, in_plane)
        send_plane(-d, 2 * d - 1, in_plane)
        if forward:
            fill_both(d + 1)

    def send_planes(first, last):
        def one(d, carry):
            send_both(d, True)
            return carry

        lax.fori_loop(first, min(last + 1, far - 1), one, 0)
        if last == far - 1:
            send_both(last, False)

    ways = [(0, quarter), (1, -quarter)]
    crossing = [(way, dz, dxl) for way, dz in ways for dxl in range(X_LO)]

    def via(src, dst, s_sem, r_sem, dz):
        pltpu.make_async_remote_copy(
            src_ref=src,
            dst_ref=dst,
            send_sem=s_sem,
            recv_sem=r_sem,
            device_id=(me_o, rep_at(dz, 0, 0)),
            device_id_type=MESH,
        ).start()

    fill_plane(far)
    send_planes(1, quarter)
    for way, dz, dxl in crossing:
        r = rep_at(far, dxl, way)
        via(
            send.at[pl.ds(r * 2 * CAP, 2 * CAP)],
            relay_rows.at[pl.ds((way * X_LO + dxl) * 2 * CAP, 2 * CAP)],
            a2a_send,
            relay_in,
            dz,
        )
    if quarter < far - 1:
        send_planes(quarter + 1, far - 1)

    def whole(buffer, sem, count):
        view = buffer.at[pl.ds(0, count)]
        return pltpu.make_async_copy(view, view, sem)

    def pass_rows():
        whole(relay_rows, relay_in, len(crossing) * 2 * CAP).wait()
        for way, dz, dxl in crossing:
            place = (n_z - 1) * plane + dxl * CORES + way
            pltpu.make_async_remote_copy(
                src_ref=relay_rows.at[pl.ds((way * X_LO + dxl) * 2 * CAP, 2 * CAP)],
                dst_ref=recv.at[pl.ds(place * 2 * CAP, 2 * CAP)],
                send_sem=relay_out,
                recv_sem=a2a_recv.at[1],
                device_id=(me_o, rep_at(dz, dxl, way)),
                device_id_type=MESH,
            ).start()

    def pass_back():
        whole(relay_back, relay_back_in, len(crossing) * CAP).wait()
        for way, dz, dxl in crossing:
            pltpu.make_async_remote_copy(
                src_ref=relay_back.at[pl.ds((way * X_LO + dxl) * CAP, CAP)],
                dst_ref=returned.at[pl.ds(rep_at(-dz, 0, 0) * CAP, CAP)],
                send_sem=relay_back_out,
                recv_sem=ret_recv,
                device_id=(me_o, rep_at(dz, dxl, way)),
                device_id_type=MESH,
            ).start()

    partner_copy.wait()
    for way in (0, 1):
        if (way, 0, True) in ring_hops(0):
            ring_copy(way, 0, True).start()
    for s in range(half):
        for way, s_, other in ring_hops(s):
            ring_copy(way, s, other).wait_recv()
            if s + 1 < half and (way, s + 1, other) in ring_hops(s + 1):
                ring_copy(way, s + 1, other).start()
        if s == half // 2 - 1:
            pass_rows()

    def forward(g):
        def widen(r, carry):
            block = recv[pl.ds((g * group + r) * 2 * CAP, 2 * CAP)].astype(jnp.float32)
            for c in range(CAP):
                at = pl.ds(pl.multiple_of((r * CAP + c) * n_own, n_own), n_own)
                wide[0, at, :] = block[c]
                wide[1, at, :] = block[CAP + c]
            return carry

        lax.fori_loop(0, group, widen, 0, unroll=2)
        mine = pl.ds(g * rows, rows)
        gate = jnp.zeros((rows, hw), jnp.float32)
        up = jnp.zeros_like(gate)
        grad_back = jnp.zeros_like(gate)
        for p in range(n_y):
            pair = []
            for i, kept in enumerate((xs, dys)):
                parts = []
                for h in range(X_HI):
                    j = X_HI * p + h
                    part = wide[i, pl.ds(j, rows, stride=n_own), :].astype(jnp.bfloat16)
                    kept[j, mine, :] = part
                    parts.append(part)
                pair.append(jnp.concatenate(parts, axis=1))
            w_of = [
                jnp.concatenate([weights[X_HI * p + h, k] for h in range(X_HI)], axis=0)
                for k in range(3)
            ]
            gate += nn(pair[0], w_of[0])
            up += nn(pair[0], w_of[1])
            grad_back += nn(pair[1], w_of[2])
        sg = jax.nn.sigmoid(gate)
        silu = gate * sg
        hidden_s[mine, :] = (silu * up).astype(jnp.bfloat16)
        grads_h[mine, :hw] = (grad_back * up * sg * (1.0 + gate * (1.0 - sg))).astype(jnp.bfloat16)
        grads_h[mine, hw:] = (grad_back * silu).astype(jnp.bfloat16)

    def give_back(g):
        mine = pl.ds(g * rows, rows)
        for j in range(n_own):
            wide[0, pl.ds(j, rows, stride=n_own), :] = nt(
                grads_h[mine, :hw], weights[j, 0]
            ) + nt(grads_h[mine, hw:], weights[j, 1])

        def narrow(r, carry):
            for c in range(CAP):
                at = pl.ds(pl.multiple_of((r * CAP + c) * n_own, n_own), n_own)
                back[g * rows + r * CAP + c] = wide[0, at, :].astype(jnp.bfloat16)
            return carry

        lax.fori_loop(0, group, narrow, 0, unroll=2)

        def home(at, dz, members):
            for dxl, dc in members:
                place = at * plane + dxl * CORES + dc
                pltpu.make_async_remote_copy(
                    src_ref=back.at[pl.ds(place * CAP, CAP)],
                    dst_ref=returned.at[pl.ds(me_r * CAP, CAP)],
                    send_sem=ret_send,
                    recv_sem=ret_recv,
                    device_id=(me_o, rep_at(dz, dxl, dc)),
                    device_id_type=MESH,
                ).start()

        def homes(at, carry):
            up_z = (at + 1) // 2
            home(at, jnp.where(lax.rem(at, 2) == 1, up_z, -up_z), in_plane)
            return carry

        if g == 0:
            home(0, 0, in_plane[1:])
            lax.fori_loop(1, far, homes, 0)
            return
        for way, dz, dxl in crossing:
            place = (n_z - 1) * plane + dxl * CORES + way
            via(
                back.at[pl.ds(place * CAP, CAP)],
                relay_back.at[pl.ds((way * X_LO + dxl) * CAP, CAP)],
                ret_send,
                relay_back_in,
                dz,
            )
        lax.fori_loop(far, n_z - 1, homes, 0)

    self_copy.wait()
    whole(recv, a2a_recv.at[0], (group - 1) * 2 * CAP).wait()
    forward(0)
    give_back(0)
    back_copy = pltpu.make_async_copy(
        back.at[pl.ds(0, CAP)], returned.at[pl.ds(me_r * CAP, CAP)], local_sem.at[0]
    )
    back_copy.start()
    whole(recv, a2a_recv.at[1], group * 2 * CAP).wait()
    forward(1)

    def terms(dy, column):
        j = own_at(dy, xh if column else 1 - xh)
        both = tn(xs[j], grads_h[...])
        return both[:, :hw], both[:, hw:], tn(dys[j], hidden_s[...])

    size = wg_ref.shape[1]
    lead = early.shape[2]

    def bounds(way, s, column):
        low = 0 if column else lead
        if s:
            return low, size
        middle = (low + size) // 2
        return ((low, middle), (middle, size))[way]

    def sum_copy(way, s, column):
        low, high = bounds(way, s, column)
        part = (way, s, column, slice(None), pl.ds(low, high - low))
        return pltpu.make_async_remote_copy(
            src_ref=stage.at[part],
            dst_ref=chain.at[part],
            send_sem=rs_send.at[way, s, column],
            recv_sem=rs_recv.at[way, s, column],
            device_id=towards[way],
            device_id_type=MESH,
        )

    def first_copy(i):
        return pltpu.make_async_remote_copy(
            src_ref=early.at[i],
            dst_ref=earlier.at[i],
            send_sem=first_send.at[i],
            recv_sem=first_recv.at[i],
            device_id=partner,
            device_id_type=MESH,
        )

    def blocks(s):
        if s == 0:
            return [(0, half, (0, 1))]
        if s == half:
            return [(2 * half - 1, 0, ())]
        return [(2 * s - 1, half - s, (0,)), (2 * s, s - half, (1,))]

    def put_terms(s, column):
        for i, dy, sides in blocks(s):
            for k, term in enumerate(terms(dy, column)):
                value = term.astype(jnp.bfloat16)
                if not column:
                    early[i, k] = value[:lead]
                for way in sides:
                    low, high = bounds(way, s, column)
                    stage[way, s, column, k, low:high] = value[low:high]
                if not sides:
                    total[column, k] = value.astype(jnp.float32)
            if not column:
                first_copy(i).start()

    def add_to(way, s, column, k, low, high, more):
        stage[way, s, column, k, low:high] = (
            stage[way, s, column, k, low:high].astype(jnp.float32) + more.astype(jnp.float32)
        ).astype(jnp.bfloat16)

    def send_sums(s, column):
        for i, dy, sides in blocks(s):
            for way in sides:
                if column and bounds(way, s, column)[0] == 0:
                    first_copy(i).wait_recv()
                    for k in range(3):
                        add_to(way, s, column, k, 0, lead, earlier[i, k])
                if s:
                    sum_copy(way, s - 1, column).wait_recv()
                    low, high = bounds(way, s - 1, column)
                    for k in range(3):
                        add_to(way, s, column, k, low, high, chain[way, s - 1, column, k, low:high])
                sum_copy(way, s, column).start()

    put_terms(0, 0)
    send_sums(0, 0)
    give_back(1)
    put_terms(0, 1)
    put_terms(1, 0)
    send_sums(0, 1)
    for s in range(1, half):
        put_terms(s, 1)
        send_sums(s, 0)
        put_terms(s + 1, 0)
        send_sums(s, 1)
        if s == min(2, half - 1):
            pass_back()
    put_terms(half, 1)

    def summed(column, k, low):
        value = total[column, k, low:]
        for way in (0, 1):
            value += chain[way, half - 1, column, k, low:].astype(jnp.float32)
        return value

    for way in (0, 1):
        sum_copy(way, half - 1, 0).wait_recv()
    for k in range(3):
        cross[k, lead:] = summed(0, k, lead).astype(jnp.bfloat16)
    later = (slice(None), pl.ds(lead, size - lead))
    cross_copy = pltpu.make_async_remote_copy(
        src_ref=cross.at[later],
        dst_ref=crossed.at[later],
        send_sem=rsx_send,
        recv_sem=rsx_recv,
        device_id=partner,
        device_id_type=MESH,
    )
    cross_copy.start()
    for way in (0, 1):
        sum_copy(way, half - 1, 1).wait_recv()
    first_copy(2 * half - 1).wait_recv()
    for k in range(3):
        total[1, k] = summed(1, k, 0)
        sums_ref[k, :lead] = total[1, k, :lead] + earlier[2 * half - 1, k].astype(jnp.float32)

    back_copy.wait()
    whole(returned, ret_recv, (n_rep - 1) * CAP).wait()

    def pick(t, carry):
        xg_ref[t] = returned[jnp.clip(index[1, t], 0, n_rep * CAP - 1)]
        return carry

    lax.fori_loop(0, toks, pick, 0, unroll=8)

    cross_copy.wait()
    for k in range(3):
        sums_ref[k, lead:] = total[1, k, lead:] + crossed[k, lead:].astype(jnp.float32)

    whole(send, a2a_send, (n_rep - 1) * 2 * CAP).wait()
    whole(back, ret_send, (n_rep - 1) * CAP).wait()
    whole(relay_rows, relay_out, len(crossing) * 2 * CAP).wait()
    whole(relay_back, relay_back_out, len(crossing) * CAP).wait()
    for s in range(half):
        for way, s_, other in ring_hops(s):
            ring_copy(way, s, other).wait_send()
        for way in (0, 1):
            for column in range(X_HI):
                sum_copy(way, s, column).wait_send()
    for i in range(2 * half):
        first_copy(i).wait_send()


def shards(n_own, n_rep, tokens, cotangent, route, host, w_gate, w_up, w_down_t):
    tok_rows, width = tokens.shape
    hw = w_gate.shape[2]
    piece = w_gate.shape[1]
    lanes = width // n_own
    rows = n_rep * CAP
    bf16, f32 = jnp.bfloat16, jnp.float32
    half = n_own // X_HI // 2
    vmem = pl.BlockSpec(memory_space=pltpu.VMEM)
    table = (2, -(-max(rows, tok_rows) // 128) * 128)
    anywhere = pl.BlockSpec(memory_space=pl.ANY)
    dma = pltpu.SemaphoreType.DMA
    x_rows, sums = pl.pallas_call(
        functools.partial(kernel, n_own, n_rep),
        out_shape=(
            jax.ShapeDtypeStruct((tok_rows, n_own, lanes), bf16),
            jax.ShapeDtypeStruct((3, piece, hw), f32),
        ),
        in_specs=[anywhere] * 7,
        out_specs=(vmem,) * 2,
        scratch_shapes=[
            pltpu.VMEM((1, tok_rows), jnp.int32),
            pltpu.VMEM((1, n_rep), jnp.int32),
            pltpu.VMEM(table, jnp.int32),
            pltpu.SMEM(table, jnp.int32),
            pltpu.VMEM((2, tok_rows, width), bf16),
            pltpu.VMEM((tok_rows + 1, n_own, lanes), bf16),
            pltpu.VMEM((tok_rows + 1, n_own, lanes), bf16),
            pltpu.VMEM((2 * rows, n_own, lanes), bf16),
            pltpu.VMEM((2 * rows, n_own, lanes), bf16),
            pltpu.VMEM((n_own, 3, piece, hw), bf16),
            pltpu.VMEM((2, max(rows // 2, tok_rows) * n_own, lanes), f32),
            pltpu.VMEM((n_own, rows, lanes), bf16),
            pltpu.VMEM((n_own, rows, lanes), bf16),
            pltpu.VMEM((rows, 2 * hw), bf16),
            pltpu.VMEM((rows, hw), bf16),
            pltpu.VMEM((rows, n_own, lanes), bf16),
            pltpu.VMEM((rows, n_own, lanes), bf16),
            pltpu.VMEM((2, half, X_HI, 3, piece, hw), bf16),
            pltpu.VMEM((2, half, X_HI, 3, piece, hw), bf16),
            pltpu.VMEM((X_HI, 3, piece, hw), f32),
            pltpu.VMEM((3, piece, hw), bf16),
            pltpu.VMEM((3, piece, hw), bf16),
            pltpu.VMEM((n_own // X_HI, 3, piece // 4, hw), bf16),
            pltpu.VMEM((n_own // X_HI, 3, piece // 4, hw), bf16),
            pltpu.VMEM((4 * CAP * X_LO, n_own, lanes), bf16),
            pltpu.VMEM((2 * CAP * X_LO, n_own, lanes), bf16),
            dma((7,)),
            pltpu.SemaphoreType.REGULAR((2, n_rep // (X_LO * CORES) // 2 - 1)),
            dma,
            dma,
            dma,
            dma,
            dma,
            dma((2,)),
            dma,
            dma,
            dma,
            dma,
            dma((2, half, 2)),
            dma((2, half, 2)),
            dma((2, half, 2)),
            dma((2, half, 2)),
            dma,
            dma,
            dma((n_own // X_HI,)),
            dma((n_own // X_HI,)),
        ],
        compiler_params=pltpu.CompilerParams(collective_id=0, has_side_effects=True),
    )(route.reshape(1, tok_rows), host[None], tokens, cotangent, w_gate, w_up, w_down_t)
    return (x_rows.reshape(tok_rows, width), sums[0:1], sums[1:2], sums[2:3])


def solution(mesh):
    body = functools.partial(shards, mesh.shape["own"], mesh.shape["rep"])
    return jax.shard_map(
        body,
        mesh=mesh,
        in_specs=(
            P(("own", "rep"), None),
            P(("own", "rep"), None),
            P(("own", "rep"), None),
            P(),
            P("rep", "own", None),
            P("rep", "own", None),
            P("rep", "own", None),
        ),
        out_specs=(
            P(("own", "rep"), None),
            P("rep", "own", None),
            P("rep", "own", None),
            P("rep", "own", None),
        ),
        check_vma=False,
    )
```

```python
import functools

import jax
import jax.numpy as jnp
from jax import lax
from jax.experimental import pallas as pl
from jax.experimental.pallas import tpu as pltpu
from jax.sharding import PartitionSpec as P

MESH = pl.DeviceIdType.MESH
CAP = 3
CORES = 2
X_LO = 2
X_HI = 2


def nn(left, right):
    return lax.dot_general(
        left, right, (((1,), (0,)), ((), ())), preferred_element_type=jnp.float32
    )


def nt(left, right):
    return lax.dot_general(
        left, right, (((1,), (1,)), ((), ())), preferred_element_type=jnp.float32
    )


def tn(left, right):
    return lax.dot_general(
        left, right, (((0,), (0,)), ((), ())), preferred_element_type=jnp.float32
    )


def kernel(
    n_own,
    n_rep,
    route_ref,
    host_ref,
    tok_ref,
    cot_ref,
    wg_ref,
    wu_ref,
    wd_ref,
    xg_ref,
    sums_ref,
    route_in,
    host_in,
    table,
    index,
    tok_in,
    x_of,
    dy_of,
    send,
    recv,
    weights,
    wide,
    xs,
    dys,
    grads_h,
    hidden_s,
    back,
    returned,
    stage,
    chain,
    total,
    cross,
    crossed,
    early,
    earlier,
    relay_rows,
    relay_back,
    local_sem,
    ready,
    relay_in,
    relay_out,
    relay_back_in,
    relay_back_out,
    a2a_send,
    a2a_recv,
    ret_send,
    ret_recv,
    agx_send,
    agx_recv,
    ag_send,
    ag_recv,
    rs_send,
    rs_recv,
    rsx_send,
    rsx_recv,
    first_send,
    first_recv,
):
    n_y = n_own // X_HI
    n_z = n_rep // (X_LO * CORES)
    half = n_y // 2
    plane = X_LO * CORES
    far = n_z // 2
    quarter = n_z // 4
    group = n_rep // 2
    rows = group * CAP
    hw = wg_ref.shape[2]
    toks = tok_ref.shape[0]
    lanes = tok_ref.shape[1] // n_own
    me_o = lax.axis_index("own")
    me_r = lax.axis_index("rep")
    y = me_o // X_HI
    xh = lax.rem(me_o, X_HI)
    xl = me_r // (n_z * CORES)
    z = lax.rem(me_r // CORES, n_z)
    core = lax.rem(me_r, CORES)

    def own_at(dy, h):
        return lax.rem(y + dy + n_y, n_y) * X_HI + h

    right = (own_at(1, xh), me_r)
    left = (own_at(-1, xh), me_r)
    partner = (y * X_HI + (1 - xh), me_r)
    towards = (right, left)

    def rep_at(dz, dxl, dc):
        return (
            lax.rem(xl + dxl, X_LO) * (n_z * CORES)
            + lax.rem(z + dz + n_z, n_z) * CORES
            + lax.rem(core + dc, CORES)
        )

    def signal(sem, dev):
        pl.semaphore_signal(sem, inc=1, device_id=dev, device_id_type=MESH)

    in_plane = [(dxl, dc) for dxl in range(X_LO) for dc in range(CORES)]
    ahead = (me_o, rep_at(1, 0, 0))
    behind = (me_o, rep_at(-1, 0, 0))
    barrier = pltpu.get_barrier_semaphore()
    for dev in (right, left, partner, ahead, behind):
        signal(barrier, dev)
    for dxl, dc in in_plane[1:]:
        signal(barrier, (me_o, rep_at(0, dxl, dc)))

    names = [
        pltpu.make_async_copy(route_ref, route_in, local_sem.at[5]),
        pltpu.make_async_copy(host_ref, host_in, local_sem.at[6]),
    ]
    loads = [
        pltpu.make_async_copy(ref, tok_in.at[i], local_sem.at[3 + i])
        for i, ref in enumerate((tok_ref, cot_ref))
    ] + [
        pltpu.make_async_copy(w_ref.at[0], weights.at[me_o, k], local_sem.at[k])
        for k, w_ref in enumerate((wg_ref, wu_ref, wd_ref))
    ]
    for copy in names + loads:
        copy.start()

    for copy in names:
        copy.wait()
    def across(shape, axis):
        return lax.broadcasted_iota(jnp.int32, shape, axis)

    def turned(row, size):
        eye = across((size, row.shape[1]), 0) == across((size, row.shape[1]), 1)
        return jnp.sum(jnp.where(eye, row, 0), axis=1, keepdims=True)

    route_row = route_in[...]
    host_col = turned(host_in[...], n_rep)
    named = across((n_rep, toks), 0) == route_row
    target_row = jnp.sum(jnp.where(named, host_col, 0), axis=0, keepdims=True)
    square = (toks, toks)
    same = (turned(target_row, toks) == target_row) & (across(square, 0) < across(square, 1))
    arrival_row = jnp.sum(jnp.where(same, 1, 0), axis=0, keepdims=True)
    position_row = target_row * CAP + arrival_row
    slots = index.shape[1]
    spread = (toks, slots)
    holds = turned(position_row, toks) == across(spread, 1)
    source_row = toks + jnp.sum(
        jnp.where(holds, across(spread, 0) - toks, 0), axis=0, keepdims=True
    )
    table[0:1, :] = source_row
    table[1:2, 0:toks] = position_row
    to_scalars = pltpu.make_async_copy(table, index, local_sem.at[5])
    to_scalars.start()

    for i in range(2):
        loads[i].wait()
        for j in range(n_own):
            wide[i, pl.ds(j, toks, stride=n_own), :] = tok_in[
                i, :, j * lanes : (j + 1) * lanes
            ].astype(jnp.float32)

    def by_token(t, carry):
        at = pl.ds(pl.multiple_of(t * n_own, n_own), n_own)
        x_of[t] = wide[0, at, :].astype(jnp.bfloat16)
        dy_of[t] = wide[1, at, :].astype(jnp.bfloat16)
        return carry

    lax.fori_loop(0, toks, by_token, 0, unroll=16)
    for rows_of in (x_of, dy_of):
        rows_of[toks] = jnp.zeros((n_own, lanes), jnp.bfloat16)

    def fill_plane(dz):
        for dxl, dc in in_plane:
            r = rep_at(dz, dxl, dc)
            for c in range(CAP):
                row = jnp.clip(index[0, r * CAP + c], 0, toks)
                send[r * 2 * CAP + c] = x_of[row]
                send[r * 2 * CAP + CAP + c] = dy_of[row]

    def fill_both(d):
        fill_plane(d)
        fill_plane(-d)

    to_scalars.wait()
    fill_plane(0)
    fill_both(1)
    for copy in loads[2:]:
        copy.wait()
    pl.semaphore_wait(barrier, 5 + plane - 1)

    signal(ready.at[0, 0], ahead)
    signal(ready.at[1, 0], behind)

    def weight_copy(block, dev, s_sem, r_sem):
        return pltpu.make_async_remote_copy(
            src_ref=weights.at[block],
            dst_ref=weights.at[block],
            send_sem=s_sem,
            recv_sem=r_sem,
            device_id=dev,
            device_id_type=MESH,
        )

    partner_copy = weight_copy(me_o, partner, agx_send, agx_recv)
    partner_copy.start()

    def ring_copy(way, s, other):
        h = (1 - xh) if other else xh
        block = own_at(-s if way == 0 else s, h)
        return weight_copy(
            block,
            towards[way],
            ag_send.at[way, s, int(other)],
            ag_recv.at[way, s, int(other)],
        )

    def ring_hops(s):
        if s < half - 1:
            return [(way, s, other) for other in (False, True) for way in (0, 1)]
        return [(0, s, False), (1, s, True)]

    for way in (0, 1):
        if (way, 0, False) in ring_hops(0):
            ring_copy(way, 0, False).start()

    def send_plane(dz, at, members):
        for dxl, dc in members:
            r = rep_at(dz, dxl, dc)
            place = at * plane + dxl * CORES + dc
            pltpu.make_async_remote_copy(
                src_ref=send.at[pl.ds(r * 2 * CAP, 2 * CAP)],
                dst_ref=recv.at[pl.ds(place * 2 * CAP, 2 * CAP)],
                send_sem=a2a_send,
                recv_sem=a2a_recv.at[at // far],
                device_id=(me_o, r),
                device_id_type=MESH,
            ).start()

    send_plane(0, 0, in_plane[1:])
    self_copy = pltpu.make_async_copy(
        send.at[pl.ds(me_r * 2 * CAP, 2 * CAP)],
        recv.at[pl.ds(0, 2 * CAP)],
        local_sem.at[0],
    )
    self_copy.start()

    def send_both(d, forward):
        for way, ahead_of in enumerate((ahead, behind)):
            pl.semaphore_wait(ready.at[way, d - 1], 1)
            if forward:
                signal(ready.at[way, d], ahead_of)
        send_plane(d, 2 * d, in_plane)
        send_plane(-d, 2 * d - 1, in_plane)
        if forward:
            fill_both(d + 1)

    def send_planes(first, last):
        def one(d, carry):
            send_both(d, True)
            return carry

        lax.fori_loop(first, min(last + 1, far - 1), one, 0)
        if last == far - 1:
            send_both(last, False)

    ways = [(0, quarter), (1, -quarter)]
    crossing = [(way, dz, dxl) for way, dz in ways for dxl in range(X_LO)]

    def via(src, dst, s_sem, r_sem, dz):
        pltpu.make_async_remote_copy(
            src_ref=src,
            dst_ref=dst,
            send_sem=s_sem,
            recv_sem=r_sem,
            device_id=(me_o, rep_at(dz, 0, 0)),
            device_id_type=MESH,
        ).start()

    fill_plane(far)
    send_planes(1, quarter)
    for way, dz, dxl in crossing:
        r = rep_at(far, dxl, way)
        via(
            send.at[pl.ds(r * 2 * CAP, 2 * CAP)],
            relay_rows.at[pl.ds((way * X_LO + dxl) * 2 * CAP, 2 * CAP)],
            a2a_send,
            relay_in,
            dz,
        )
    if quarter < far - 1:
        send_planes(quarter + 1, far - 1)

    def whole(buffer, sem, count):
        view = buffer.at[pl.ds(0, count)]
        return pltpu.make_async_copy(view, view, sem)

    def pass_rows():
        whole(relay_rows, relay_in, len(crossing) * 2 * CAP).wait()
        for way, dz, dxl in crossing:
            place = (n_z - 1) * plane + dxl * CORES + way
            pltpu.make_async_remote_copy(
                src_ref=relay_rows.at[pl.ds((way * X_LO + dxl) * 2 * CAP, 2 * CAP)],
                dst_ref=recv.at[pl.ds(place * 2 * CAP, 2 * CAP)],
                send_sem=relay_out,
                recv_sem=a2a_recv.at[1],
                device_id=(me_o, rep_at(dz, dxl, way)),
                device_id_type=MESH,
            ).start()

    def pass_back():
        whole(relay_back, relay_back_in, len(crossing) * CAP).wait()
        for way, dz, dxl in crossing:
            pltpu.make_async_remote_copy(
                src_ref=relay_back.at[pl.ds((way * X_LO + dxl) * CAP, CAP)],
                dst_ref=returned.at[pl.ds(rep_at(-dz, 0, 0) * CAP, CAP)],
                send_sem=relay_back_out,
                recv_sem=ret_recv,
                device_id=(me_o, rep_at(dz, dxl, way)),
                device_id_type=MESH,
            ).start()

    partner_copy.wait()
    for way in (0, 1):
        if (way, 0, True) in ring_hops(0):
            ring_copy(way, 0, True).start()
    for s in range(half):
        for way, s_, other in ring_hops(s):
            ring_copy(way, s, other).wait_recv()
            if s + 1 < half and (way, s + 1, other) in ring_hops(s + 1):
                ring_copy(way, s + 1, other).start()
        if s == half // 2 - 1:
            pass_rows()

    def forward(g):
        def widen(r, carry):
            block = recv[pl.ds((g * group + r) * 2 * CAP, 2 * CAP)].astype(jnp.float32)
            for c in range(CAP):
                at = pl.ds(pl.multiple_of((r * CAP + c) * n_own, n_own), n_own)
                wide[0, at, :] = block[c]
                wide[1, at, :] = block[CAP + c]
            return carry

        lax.fori_loop(0, group, widen, 0, unroll=2)
        mine = pl.ds(g * rows, rows)
        gate = jnp.zeros((rows, hw), jnp.float32)
        up = jnp.zeros_like(gate)
        grad_back = jnp.zeros_like(gate)
        for p in range(n_y):
            pair = []
            for i, kept in enumerate((xs, dys)):
                parts = []
                for h in range(X_HI):
                    j = X_HI * p + h
                    part = wide[i, pl.ds(j, rows, stride=n_own), :].astype(jnp.bfloat16)
                    kept[j, mine, :] = part
                    parts.append(part)
                pair.append(jnp.concatenate(parts, axis=1))
            w_of = [
                jnp.concatenate([weights[X_HI * p + h, k] for h in range(X_HI)], axis=0)
                for k in range(3)
            ]
            gate += nn(pair[0], w_of[0])
            up += nn(pair[0], w_of[1])
            grad_back += nn(pair[1], w_of[2])
        sg = jax.nn.sigmoid(gate)
        silu = gate * sg
        hidden_s[mine, :] = (silu * up).astype(jnp.bfloat16)
        grads_h[mine, :hw] = (grad_back * up * sg * (1.0 + gate * (1.0 - sg))).astype(jnp.bfloat16)
        grads_h[mine, hw:] = (grad_back * silu).astype(jnp.bfloat16)

    def give_back(g):
        mine = pl.ds(g * rows, rows)
        for j in range(n_own):
            wide[0, pl.ds(j, rows, stride=n_own), :] = nt(
                grads_h[mine, :hw], weights[j, 0]
            ) + nt(grads_h[mine, hw:], weights[j, 1])

        def narrow(r, carry):
            for c in range(CAP):
                at = pl.ds(pl.multiple_of((r * CAP + c) * n_own, n_own), n_own)
                back[g * rows + r * CAP + c] = wide[0, at, :].astype(jnp.bfloat16)
            return carry

        lax.fori_loop(0, group, narrow, 0, unroll=2)

        def home(at, dz, members):
            for dxl, dc in members:
                place = at * plane + dxl * CORES + dc
                pltpu.make_async_remote_copy(
                    src_ref=back.at[pl.ds(place * CAP, CAP)],
                    dst_ref=returned.at[pl.ds(me_r * CAP, CAP)],
                    send_sem=ret_send,
                    recv_sem=ret_recv,
                    device_id=(me_o, rep_at(dz, dxl, dc)),
                    device_id_type=MESH,
                ).start()

        def homes(at, carry):
            up_z = (at + 1) // 2
            home(at, jnp.where(lax.rem(at, 2) == 1, up_z, -up_z), in_plane)
            return carry

        if g == 0:
            home(0, 0, in_plane[1:])
            lax.fori_loop(1, far, homes, 0)
            return
        for way, dz, dxl in crossing:
            place = (n_z - 1) * plane + dxl * CORES + way
            via(
                back.at[pl.ds(place * CAP, CAP)],
                relay_back.at[pl.ds((way * X_LO + dxl) * CAP, CAP)],
                ret_send,
                relay_back_in,
                dz,
            )
        lax.fori_loop(far, n_z - 1, homes, 0)

    self_copy.wait()
    whole(recv, a2a_recv.at[0], (group - 1) * 2 * CAP).wait()
    forward(0)
    give_back(0)
    back_copy = pltpu.make_async_copy(
        back.at[pl.ds(0, CAP)], returned.at[pl.ds(me_r * CAP, CAP)], local_sem.at[0]
    )
    back_copy.start()
    whole(recv, a2a_recv.at[1], group * 2 * CAP).wait()
    forward(1)

    def terms(dy, column):
        j = own_at(dy, xh if column else 1 - xh)
        both = tn(xs[j], grads_h[...])
        return both[:, :hw], both[:, hw:], tn(dys[j], hidden_s[...])

    size = wg_ref.shape[1]
    lead = early.shape[2]

    def bounds(way, s, column):
        low = 0 if column else lead
        if s:
            return low, size
        middle = (low + size) // 2
        return ((low, middle), (middle, size))[way]

    def sum_copy(way, s, column):
        low, high = bounds(way, s, column)
        part = (way, s, column, slice(None), pl.ds(low, high - low))
        return pltpu.make_async_remote_copy(
            src_ref=stage.at[part],
            dst_ref=chain.at[part],
            send_sem=rs_send.at[way, s, column],
            recv_sem=rs_recv.at[way, s, column],
            device_id=towards[way],
            device_id_type=MESH,
        )

    def first_copy(i):
        return pltpu.make_async_remote_copy(
            src_ref=early.at[i],
            dst_ref=earlier.at[i],
            send_sem=first_send.at[i],
            recv_sem=first_recv.at[i],
            device_id=partner,
            device_id_type=MESH,
        )

    def blocks(s):
        if s == 0:
            return [(0, half, (0, 1))]
        if s == half:
            return [(2 * half - 1, 0, ())]
        return [(2 * s - 1, half - s, (0,)), (2 * s, s - half, (1,))]

    def put_terms(s, column):
        for i, dy, sides in blocks(s):
            for k, term in enumerate(terms(dy, column)):
                value = term.astype(jnp.bfloat16)
                if not column:
                    early[i, k] = value[:lead]
                for way in sides:
                    low, high = bounds(way, s, column)
                    stage[way, s, column, k, low:high] = value[low:high]
                if not sides:
                    total[column, k] = value.astype(jnp.float32)
            if not column:
                first_copy(i).start()

    def add_to(way, s, column, k, low, high, more):
        stage[way, s, column, k, low:high] = (
            stage[way, s, column, k, low:high].astype(jnp.float32) + more.astype(jnp.float32)
        ).astype(jnp.bfloat16)

    def send_sums(s, column):
        for i, dy, sides in blocks(s):
            for way in sides:
                if column and bounds(way, s, column)[0] == 0:
                    first_copy(i).wait_recv()
                    for k in range(3):
                        add_to(way, s, column, k, 0, lead, earlier[i, k])
                if s:
                    sum_copy(way, s - 1, column).wait_recv()
                    low, high = bounds(way, s - 1, column)
                    for k in range(3):
                        add_to(way, s, column, k, low, high, chain[way, s - 1, column, k, low:high])
                sum_copy(way, s, column).start()

    put_terms(0, 0)
    send_sums(0, 0)
    give_back(1)
    put_terms(0, 1)
    put_terms(1, 0)
    send_sums(0, 1)
    for s in range(1, half):
        put_terms(s, 1)
        send_sums(s, 0)
        put_terms(s + 1, 0)
        send_sums(s, 1)
        if s == min(2, half - 1):
            pass_back()
    put_terms(half, 1)

    def summed(column, k, low):
        value = total[column, k, low:]
        for way in (0, 1):
            value += chain[way, half - 1, column, k, low:].astype(jnp.float32)
        return value

    for way in (0, 1):
        sum_copy(way, half - 1, 0).wait_recv()
    for k in range(3):
        cross[k, lead:] = summed(0, k, lead).astype(jnp.bfloat16)
    later = (slice(None), pl.ds(lead, size - lead))
    cross_copy = pltpu.make_async_remote_copy(
        src_ref=cross.at[later],
        dst_ref=crossed.at[later],
        send_sem=rsx_send,
        recv_sem=rsx_recv,
        device_id=partner,
        device_id_type=MESH,
    )
    cross_copy.start()
    for way in (0, 1):
        sum_copy(way, half - 1, 1).wait_recv()
    first_copy(2 * half - 1).wait_recv()
    for k in range(3):
        total[1, k] = summed(1, k, 0)
        sums_ref[k, :lead] = total[1, k, :lead] + earlier[2 * half - 1, k].astype(jnp.float32)

    back_copy.wait()
    whole(returned, ret_recv, (n_rep - 1) * CAP).wait()

    def pick(t, carry):
        at = pl.ds(pl.multiple_of(t * n_own, n_own), n_own)
        row = returned[jnp.clip(index[1, t], 0, n_rep * CAP - 1)]
        wide[0, at, :] = row.astype(jnp.float32)
        return carry

    lax.fori_loop(0, toks, pick, 0, unroll=8)
    for j in range(n_own):
        xg_ref[:, j * lanes : (j + 1) * lanes] = wide[
            0, pl.ds(j, toks, stride=n_own), :
        ].astype(jnp.bfloat16)

    cross_copy.wait()
    for k in range(3):
        sums_ref[k, lead:] = total[1, k, lead:] + crossed[k, lead:].astype(jnp.float32)

    whole(send, a2a_send, (n_rep - 1) * 2 * CAP).wait()
    whole(back, ret_send, (n_rep - 1) * CAP).wait()
    whole(relay_rows, relay_out, len(crossing) * 2 * CAP).wait()
    whole(relay_back, relay_back_out, len(crossing) * CAP).wait()
    for s in range(half):
        for way, s_, other in ring_hops(s):
            ring_copy(way, s, other).wait_send()
        for way in (0, 1):
            for column in range(X_HI):
                sum_copy(way, s, column).wait_send()
    for i in range(2 * half):
        first_copy(i).wait_send()


def shards(n_own, n_rep, tokens, cotangent, route, host, w_gate, w_up, w_down_t):
    tok_rows, width = tokens.shape
    hw = w_gate.shape[2]
    piece = w_gate.shape[1]
    lanes = width // n_own
    rows = n_rep * CAP
    bf16, f32 = jnp.bfloat16, jnp.float32
    half = n_own // X_HI // 2
    vmem = pl.BlockSpec(memory_space=pltpu.VMEM)
    table = (2, -(-max(rows, tok_rows) // 128) * 128)
    anywhere = pl.BlockSpec(memory_space=pl.ANY)
    dma = pltpu.SemaphoreType.DMA
    x_rows, sums = pl.pallas_call(
        functools.partial(kernel, n_own, n_rep),
        out_shape=(
            jax.ShapeDtypeStruct((tok_rows, width), bf16),
            jax.ShapeDtypeStruct((3, piece, hw), f32),
        ),
        in_specs=[anywhere] * 7,
        out_specs=(vmem,) * 2,
        scratch_shapes=[
            pltpu.VMEM((1, tok_rows), jnp.int32),
            pltpu.VMEM((1, n_rep), jnp.int32),
            pltpu.VMEM(table, jnp.int32),
            pltpu.SMEM(table, jnp.int32),
            pltpu.VMEM((2, tok_rows, width), bf16),
            pltpu.VMEM((tok_rows + 1, n_own, lanes), bf16),
            pltpu.VMEM((tok_rows + 1, n_own, lanes), bf16),
            pltpu.VMEM((2 * rows, n_own, lanes), bf16),
            pltpu.VMEM((2 * rows, n_own, lanes), bf16),
            pltpu.VMEM((n_own, 3, piece, hw), bf16),
            pltpu.VMEM((2, max(rows // 2, tok_rows) * n_own, lanes), f32),
            pltpu.VMEM((n_own, rows, lanes), bf16),
            pltpu.VMEM((n_own, rows, lanes), bf16),
            pltpu.VMEM((rows, 2 * hw), bf16),
            pltpu.VMEM((rows, hw), bf16),
            pltpu.VMEM((rows, n_own, lanes), bf16),
            pltpu.VMEM((rows, n_own, lanes), bf16),
            pltpu.VMEM((2, half, X_HI, 3, piece, hw), bf16),
            pltpu.VMEM((2, half, X_HI, 3, piece, hw), bf16),
            pltpu.VMEM((X_HI, 3, piece, hw), f32),
            pltpu.VMEM((3, piece, hw), bf16),
            pltpu.VMEM((3, piece, hw), bf16),
            pltpu.VMEM((n_own // X_HI, 3, piece // 4, hw), bf16),
            pltpu.VMEM((n_own // X_HI, 3, piece // 4, hw), bf16),
            pltpu.VMEM((4 * CAP * X_LO, n_own, lanes), bf16),
            pltpu.VMEM((2 * CAP * X_LO, n_own, lanes), bf16),
            dma((7,)),
            pltpu.SemaphoreType.REGULAR((2, n_rep // (X_LO * CORES) // 2 - 1)),
            dma,
            dma,
            dma,
            dma,
            dma,
            dma((2,)),
            dma,
            dma,
            dma,
            dma,
            dma((2, half, 2)),
            dma((2, half, 2)),
            dma((2, half, 2)),
            dma((2, half, 2)),
            dma,
            dma,
            dma((n_own // X_HI,)),
            dma((n_own // X_HI,)),
        ],
        compiler_params=pltpu.CompilerParams(collective_id=0, has_side_effects=True),
    )(route.reshape(1, tok_rows), host[None], tokens, cotangent, w_gate, w_up, w_down_t)
    return (x_rows, sums[0:1], sums[1:2], sums[2:3])


def solution(mesh):
    body = functools.partial(shards, mesh.shape["own"], mesh.shape["rep"])
    return jax.shard_map(
        body,
        mesh=mesh,
        in_specs=(
            P(("own", "rep"), None),
            P(("own", "rep"), None),
            P(("own", "rep"), None),
            P(),
            P("rep", "own", None),
            P("rep", "own", None),
            P("rep", "own", None),
        ),
        out_specs=(
            P(("own", "rep"), None),
            P("rep", "own", None),
            P("rep", "own", None),
            P("rep", "own", None),
        ),
        check_vma=False,
    )
```
